8 devices in a mesh: dp: 1 (over z), ep: 8 (over y, x, core).
Axes of the slice: x: 2, y: 2, z: 1, core: 2. Of those that a mesh axis runs over, the one named last changes fastest.
Arguments:
- tokens: bfloat16 [8192, 2560], P(('dp', 'ep'))
- expert_ids: int32 [8192, 6], P(('dp', 'ep'))
- gate_wts: float32 [8192, 6], P(('dp', 'ep'))
- slot_ids: int32 [8192, 6], P(('dp', 'ep'))
- w_gate: bfloat16 [64, 2560, 1536], P('ep')
- w_up: bfloat16 [64, 2560, 1536], P('ep')
- w_down: bfloat16 [64, 1536, 2560], P('ep')
Outputs:
- output: bfloat16 [8192, 2560], P(('dp', 'ep'))
All inputs are finite; a program needn't handle non-finite values.
Results may differ from the reference program's by a relative error of at most 0.001.
Values are sent between devices in bfloat16 or wider.
A program may use at most 1 GiB of HBM per device.

```python
import jax
import jax.numpy as jnp
from jax import lax

GROUP_SIZE = 8
TOK_DEV = 1024
D_MODEL = 2560
FF_DIM = 1536
EXPERTS = 64
TOP_K = 6

TOKENS = GROUP_SIZE * TOK_DEV
SHARD_CAP = 3 * TOK_DEV * TOP_K // (2 * EXPERTS)
CAPACITY = GROUP_SIZE * SHARD_CAP


def draw_routing(route_key, relabel_key):
    relabel = jax.random.permutation(relabel_key, EXPERTS)
    half_a = TOK_DEV // (2 * EXPERTS)
    hot_rows = 3 * half_a
    split_at = hot_rows * (EXPERTS // 2)
    tok_ids = jnp.arange(TOK_DEV)
    base_ids = jnp.where(tok_ids < split_at, tok_ids // hot_rows, EXPERTS // 2 + (tok_ids - split_at) // half_a)
    choice_off = jnp.arange(TOP_K)
    expert_axis = jnp.arange(EXPERTS)

    def one_shard(shard_num):
        shard_key = jax.random.fold_in(route_key, shard_num)
        perm_key, drop_key = jax.random.split(shard_key)
        tok_order = jax.random.permutation(perm_key, TOK_DEV)
        raw_ids = (base_ids[tok_order][:, None] + choice_off[None, :]) % EXPERTS
        drop_draw = jax.random.randint(drop_key, (TOK_DEV, TOP_K), 0, 8)
        keep_mask = (drop_draw != 0) | (raw_ids == TOP_K - 1)
        onehot = ((raw_ids.reshape(-1)[:, None] == expert_axis[None, :]) & keep_mask.reshape(-1)[:, None]).astype(jnp.int32)
        slot_rank = jnp.sum((jnp.cumsum(onehot, axis=0) - onehot) * onehot, axis=1).reshape(TOK_DEV, TOP_K)
        slot_ids = jnp.where(keep_mask, shard_num * SHARD_CAP + slot_rank, -1)
        return relabel[raw_ids].astype(jnp.int32), slot_ids.astype(jnp.int32)

    expert_ids, slot_ids = lax.map(one_shard, jnp.arange(GROUP_SIZE))
    return expert_ids.reshape(TOKENS, TOP_K), slot_ids.reshape(TOKENS, TOP_K)


def draw_weights(weight_key, shape_in, shape_out):
    def one_expert(expert_num):
        draw = jax.random.normal(jax.random.fold_in(weight_key, expert_num), (shape_in, shape_out), jnp.float32)
        return (draw * shape_in ** -0.5).astype(jnp.bfloat16)
    return lax.map(one_expert, jnp.arange(EXPERTS))


def setup_inputs(seed: int = 0, part: int = 0) -> dict:
    root_key = jax.random.key(seed)
    part_keys = jax.random.split(jax.random.fold_in(root_key, part), 4)
    weight_keys = jax.random.split(jax.random.key(seed + 1), 3)
    tokens = jax.random.normal(part_keys[0], (TOKENS, D_MODEL), jnp.float32).astype(jnp.bfloat16)
    gate_wts = jax.random.uniform(part_keys[1], (TOKENS, TOP_K), jnp.float32, minval=0.25, maxval=1.0) * TOP_K ** -0.5
    expert_ids, slot_ids = draw_routing(part_keys[2], part_keys[3])
    return {'tokens': tokens, 'expert_ids': expert_ids, 'gate_wts': gate_wts, 'slot_ids': slot_ids, 'w_gate': draw_weights(weight_keys[0], D_MODEL, FF_DIM), 'w_up': draw_weights(weight_keys[1], D_MODEL, FF_DIM), 'w_down': draw_weights(weight_keys[2], FF_DIM, D_MODEL)}


def reference(tokens, expert_ids, gate_wts, slot_ids, w_gate, w_up, w_down):
    keep_mask = slot_ids >= 0
    flat_slot = jnp.where(keep_mask, expert_ids * CAPACITY + slot_ids, EXPERTS * CAPACITY).reshape(-1)
    tok_index = jnp.broadcast_to(jnp.arange(TOKENS, dtype=jnp.int32)[:, None], expert_ids.shape).reshape(-1)
    slot_token = jnp.full((EXPERTS * CAPACITY,), TOKENS, jnp.int32).at[flat_slot].set(tok_index, mode='drop')
    slot_gate = jnp.zeros((EXPERTS * CAPACITY,), jnp.float32).at[flat_slot].set(gate_wts.reshape(-1), mode='drop')

    def expert_step(accum, scan_in):
        tok_rows, gate_rows, wg_one, wu_one, wd_one = scan_in
        buffer = jnp.take(tokens, tok_rows, axis=0, mode='fill', fill_value=0)
        h_gate = jnp.dot(buffer, wg_one, preferred_element_type=jnp.float32)
        h_up = jnp.dot(buffer, wu_one, preferred_element_type=jnp.float32)
        hidden = (jax.nn.silu(h_gate) * h_up).astype(jnp.bfloat16)
        expert_out = jnp.dot(hidden, wd_one, preferred_element_type=jnp.float32)
        accum = accum.at[tok_rows].add(expert_out * gate_rows[:, None], mode='drop')
        return accum, None

    accum, _ = lax.scan(expert_step, jnp.zeros((TOKENS, D_MODEL), jnp.float32), (slot_token.reshape(EXPERTS, CAPACITY), slot_gate.reshape(EXPERTS, CAPACITY), w_gate, w_up, w_down))
    return accum.astype(jnp.bfloat16)
```

```python
import functools
import jax
import jax.numpy as jnp
from jax import lax
from jax.experimental import pallas as pl
from jax.experimental.pallas import tpu as pltpu
from jax.sharding import PartitionSpec as P

NUM_CHUNKS = 4
MAX_ROWS = 384
ROW_STEP = 128
FF_BLOCK = 512
OUT_BLOCK = 512
ID_RADIX = 64


def expert_kernel(meta, gate, pos, digits, tok_hbm, wg_hbm, wu_hbm, wd_hbm, out_hbm,
                  tok, acc, wg, wu, wd, onehot, x, h, o, idx_v, idx_s, w_sem, tok_sem, idx_sem, out_sem):
    num_tok, d_model = tok.shape
    ff_dim = wg_hbm.shape[2]
    ff_steps = ff_dim // FF_BLOCK
    max_items = meta.shape[0] // 4
    num_items = meta[3 * max_items]

    def weight_copies(step, slot):
        e = meta[step // ff_steps]
        cols = pl.ds(pl.multiple_of((step % ff_steps) * FF_BLOCK, FF_BLOCK), FF_BLOCK)
        return (pltpu.make_async_copy(wg_hbm.at[e, :, cols], wg.at[slot], w_sem.at[slot, 0]),
                pltpu.make_async_copy(wu_hbm.at[e, :, cols], wu.at[slot], w_sem.at[slot, 1]),
                pltpu.make_async_copy(wd_hbm.at[e, cols, :], wd.at[slot], w_sem.at[slot, 2]))

    tok_copy = pltpu.make_async_copy(tok_hbm, tok, tok_sem)
    tok_copy.start()

    @pl.when(num_items > 0)
    def _():
        for cp in weight_copies(0, 0):
            cp.start()

    def zero(i, c):
        acc[pl.ds(pl.multiple_of(i * 8, 8), 8), :] = jnp.zeros((8, d_model), jnp.float32)
        return c

    lax.fori_loop(0, acc.shape[0] // 8, zero, 0)
    tok_copy.wait()

    def process(m, item, e, p0, rows):
        want = lax.broadcasted_iota(jnp.int32, (m, num_tok), 0) + p0
        onehot[:m, :] = jnp.where(want == pos[e], 1.0, 0.0).astype(jnp.bfloat16)
        parts = lax.dot_general(digits[...], onehot[:m, :], (((1,), (1,)), ((), ())), preferred_element_type=jnp.float32)
        idx = parts[0:1] * ID_RADIX + parts[1:2] + (1.0 - parts[2:3]) * num_tok
        idx_v[:, :m] = jnp.broadcast_to(idx.astype(jnp.int32), (8, m))
        idx_copy = pltpu.make_async_copy(idx_v, idx_s, idx_sem)
        idx_copy.start()

        def dispatch(nb, c):
            cols = pl.ds(pl.multiple_of(nb * OUT_BLOCK, OUT_BLOCK), OUT_BLOCK)
            x[:m, cols] = jnp.dot(onehot[:m, :], tok[:, cols], preferred_element_type=jnp.float32).astype(jnp.bfloat16)
            return c

        lax.fori_loop(0, d_model // OUT_BLOCK, dispatch, 0)

        def ff_step(f, c):
            step = item * ff_steps + f
            slot = step % 2

            @pl.when(step + 1 < num_items * ff_steps)
            def _():
                for cp in weight_copies(step + 1, 1 - slot):
                    cp.start()

            for cp in weight_copies(step, slot):
                cp.wait()

            def up(j, c):
                cols = pl.ds(pl.multiple_of(j * 256, 256), 256)
                a = jnp.dot(x[:m, :], wg[slot, :, cols], preferred_element_type=jnp.float32)
                u = jnp.dot(x[:m, :], wu[slot, :, cols], preferred_element_type=jnp.float32)
                h[:m, cols] = (jax.nn.silu(a) * u).astype(jnp.bfloat16)
                return c

            lax.fori_loop(0, FF_BLOCK // 256, up, 0)

            def down(nb, c):
                cols = pl.ds(pl.multiple_of(nb * OUT_BLOCK, OUT_BLOCK), OUT_BLOCK)
                part = jnp.dot(h[:m, :], wd[slot, :, cols], preferred_element_type=jnp.float32)

                @pl.when(f == 0)
                def _():
                    o[:m, cols] = part

                @pl.when(f != 0)
                def _():
                    o[:m, cols] += part

                return c

            lax.fori_loop(0, d_model // OUT_BLOCK, down, 0)
            return c

        lax.fori_loop(0, ff_steps, ff_step, 0)
        idx_copy.wait()

    def scatter(e, rows):
        width = 640

        def eight(i, c):
            base = pl.multiple_of(i * 8, 8)
            for half in range(2):
                t = [idx_s[0, base + half * 4 + k] for k in range(4)]
                g = [gate[e * num_tok + t[k]] for k in range(4)]
                for cb in range(d_model // width):
                    cols = slice(cb * width, (cb + 1) * width)
                    new = [acc[pl.ds(t[k], 1), cols] + o[pl.ds(base + half * 4 + k, 1), cols] * g[k] for k in range(4)]
                    for k in range(4):
                        acc[pl.ds(t[k], 1), cols] = new[k]
            return c

        lax.fori_loop(0, (rows + 7) // 8, eight, 0)

    def item_body(item, c):
        e, p0, rows = meta[item], meta[max_items + item], meta[2 * max_items + item]
        for m in range(ROW_STEP, MAX_ROWS + 1, ROW_STEP):
            @pl.when((rows > m - ROW_STEP) & (rows <= m))
            def _():
                process(m, item, e, p0, rows)

        scatter(e, rows)
        return c

    lax.fori_loop(0, num_items, item_body, 0)
    out_copy = pltpu.make_async_copy(acc.at[pl.ds(0, num_tok), :], out_hbm, out_sem)
    out_copy.start()
    out_copy.wait()


def expert_block(meta, gate, pos, digits, tok, w_gate, w_up, w_down):
    num_tok, d_model = tok.shape
    num_local, _, ff_dim = w_gate.shape
    smem = pl.BlockSpec(memory_space=pltpu.SMEM)
    vmem = pl.BlockSpec(memory_space=pltpu.VMEM)
    anym = pl.BlockSpec(memory_space=pl.ANY)
    rows = num_tok * 3 // 4
    return pl.pallas_call(
        expert_kernel,
        out_shape=jax.ShapeDtypeStruct((num_tok, d_model), jnp.float32),
        in_specs=[smem, smem, vmem, vmem, anym, anym, anym, anym],
        out_specs=anym,
        scratch_shapes=[
            pltpu.VMEM((num_tok, d_model), jnp.bfloat16),
            pltpu.VMEM((num_tok + 8, d_model), jnp.float32),
            pltpu.VMEM((2, d_model, FF_BLOCK), jnp.bfloat16),
            pltpu.VMEM((2, d_model, FF_BLOCK), jnp.bfloat16),
            pltpu.VMEM((2, FF_BLOCK, d_model), jnp.bfloat16),
            pltpu.VMEM((MAX_ROWS, num_tok), jnp.bfloat16),
            pltpu.VMEM((MAX_ROWS, d_model), jnp.bfloat16),
            pltpu.VMEM((MAX_ROWS, FF_BLOCK), jnp.bfloat16),
            pltpu.VMEM((MAX_ROWS, d_model), jnp.float32),
            pltpu.VMEM((8, MAX_ROWS), jnp.int32),
            pltpu.SMEM((8, MAX_ROWS), jnp.int32),
            pltpu.SemaphoreType.DMA((2, 3)),
            pltpu.SemaphoreType.DMA,
            pltpu.SemaphoreType.DMA,
            pltpu.SemaphoreType.DMA,
        ],
        compiler_params=pltpu.CompilerParams(vmem_limit_bytes=66_000_000),
        cost_estimate=pl.CostEstimate(flops=rows * 6 * d_model * ff_dim * 2, transcendentals=rows * ff_dim,
                                      bytes_accessed=num_local * 6 * d_model * ff_dim + num_tok * d_model * 6),
        name='expert_block',
    )(meta, gate, pos, digits, tok, w_gate, w_up, w_down)


def routing_tables(expert_ids, gate_wts, slot_ids, my_rank, num_local, group_size):
    tok_dev, top_k = expert_ids.shape
    tc = tok_dev // NUM_CHUNKS
    num_tok = group_size * tc
    key = jnp.where(slot_ids >= 0, expert_ids, -1).astype(jnp.float32).T
    packed = lax.all_gather(jnp.concatenate([key, gate_wts.T], axis=0), 'ep')
    packed = packed.reshape(group_size, 2, top_k, NUM_CHUNKS, tc).transpose(1, 3, 2, 0, 4)
    keys, gates = packed[0][:, None], packed[1][:, None]
    local = (my_rank * num_local + jnp.arange(num_local)).astype(jnp.float32)[None, :, None, None, None]
    hit = keys == local
    mask = jnp.any(hit, axis=2).reshape(NUM_CHUNKS, num_local, num_tok)
    gate = jnp.sum(jnp.where(hit, gates, 0.0), axis=2).reshape(NUM_CHUNKS, num_local * num_tok)
    gate = jnp.pad(gate, ((0, 0), (0, 128)))

    blocks = mask.astype(jnp.bfloat16).reshape(NUM_CHUNKS, num_local, num_tok // 128, 128)
    before = (jnp.arange(128)[:, None] < jnp.arange(128)[None, :]).astype(jnp.bfloat16)
    inner = jnp.einsum('cebk,kl->cebl', blocks, before, preferred_element_type=jnp.float32)
    sums = jnp.sum(blocks.astype(jnp.float32), axis=3)
    nb = num_tok // 128
    outer = jnp.sum(jnp.where(jnp.arange(nb)[:, None] < jnp.arange(nb)[None, :], sums[..., None], 0.0), axis=2)
    order = (inner + outer[..., None]).reshape(NUM_CHUNKS, num_local, num_tok)
    pos = jnp.where(mask, order, -1.0).astype(jnp.int32)

    count = jnp.sum(sums, axis=2).astype(jnp.int32)
    passes = (count + MAX_ROWS - 1) // MAX_ROWS
    upto = jnp.arange(num_local)[:, None] <= jnp.arange(num_local)[None, :]
    ends = jnp.sum(jnp.where(upto, passes[:, :, None], 0), axis=1)
    starts = ends - passes
    max_items = 32
    item = jnp.arange(max_items)
    mine = (starts[:, :, None] <= item) & (item < ends[:, :, None])
    e = jnp.sum(jnp.where(mine, jnp.arange(num_local)[:, None], 0), axis=1)
    p0 = jnp.sum(jnp.where(mine, (item - starts[:, :, None]) * MAX_ROWS, 0), axis=1)
    rows = jnp.minimum(jnp.sum(jnp.where(mine, count[:, :, None], 0), axis=1) - p0, MAX_ROWS)
    total = jnp.broadcast_to(ends[:, -1:], (NUM_CHUNKS, max_items))
    meta = jnp.concatenate([e, p0, rows, total], axis=1).astype(jnp.int32)
    return meta, gate, pos.reshape(NUM_CHUNKS, num_local, 1, num_tok)


def solution(mesh):
    group_size = mesh.shape['ep']
    row_spec = P(('dp', 'ep'), None)
    expert_spec = P('ep', None, None)

    def per_device(tokens, expert_ids, gate_wts, slot_ids, w_gate, w_up, w_down):
        my_rank = lax.axis_index('ep')
        tc = tokens.shape[0] // NUM_CHUNKS
        num_tok = group_size * tc
        gathered = [lax.all_gather(tokens[c * tc:(c + 1) * tc], 'ep', axis=0, tiled=True) for c in range(NUM_CHUNKS)]
        meta, gate, pos = routing_tables(expert_ids, gate_wts, slot_ids, my_rank, w_gate.shape[0], group_size)
        ids = jnp.arange(num_tok)
        digits = jnp.stack([ids // ID_RADIX, ids % ID_RADIX, jnp.ones_like(ids)] + [jnp.zeros_like(ids)] * 5).astype(jnp.bfloat16)
        outs = []
        for c in range(NUM_CHUNKS):
            part = expert_block(meta[c], gate[c], pos[c], digits, gathered[c], w_gate, w_up, w_down)
            outs.append(lax.psum_scatter(part, 'ep', scatter_dimension=0, tiled=True).astype(jnp.bfloat16))
        return jnp.concatenate(outs, axis=0)

    return jax.shard_map(per_device, mesh=mesh, in_specs=(row_spec, row_spec, row_spec, row_spec, expert_spec, expert_spec, expert_spec), out_specs=row_spec, check_vma=False)
```

```python
import jax
import jax.numpy as jnp
from jax import lax
from jax.experimental import pallas as pl
from jax.experimental.pallas import tpu as pltpu
from jax.sharding import PartitionSpec as P

UNIT = 128
CHUNK_UNITS = (1, 2, 2, 2, 1)
GATHERS = ((0,), (1,), (2, 3, 4))
ROW_SIZES = {1: (128, 160, 384), 2: (128, 256, 288, 384)}
MAX_ROWS = 384
MAX_ITEMS = 32
FF_BLOCK = 256
OUT_BLOCK = 512
ID_RADIX = 64
PIECES = 8


def expert_kernel(row0, row_sizes, meta, gate, pos, digits, tok_hbm, wg_hbm, wu_hbm, wd_hbm, keep_hbm, send_hbm,
                  tok, acc, wg, wu, wd, onehot, x, h, o, idx_v, idx_s, up_sem, down_sem, tok_sem, idx_sem, out_sem):
    num_tok, d_model = tok.shape
    shards = tok_hbm.shape[0]
    tc = num_tok // shards
    ff_dim = wg_hbm.shape[2]
    up_steps, down_steps = ff_dim // FF_BLOCK, d_model // OUT_BLOCK
    num_items = meta[3 * MAX_ITEMS]
    parity = meta[3 * MAX_ITEMS + 1]

    def up_copies(item, j):
        cols = pl.ds(pl.multiple_of(j * FF_BLOCK, FF_BLOCK), FF_BLOCK)
        e = meta[item]
        return (pltpu.make_async_copy(wg_hbm.at[e, :, cols], wg.at[j], up_sem.at[j, 0]),
                pltpu.make_async_copy(wu_hbm.at[e, :, cols], wu.at[j], up_sem.at[j, 1]))

    def down_copy(item, j):
        cols = pl.ds(pl.multiple_of(j * OUT_BLOCK, OUT_BLOCK), OUT_BLOCK)
        return pltpu.make_async_copy(wd_hbm.at[meta[item], :, cols], wd.at[j], down_sem.at[j])

    tok_copies = [pltpu.make_async_copy(tok_hbm.at[s, pl.ds(row0, tc), :], tok.at[pl.ds(s * tc, tc), :], tok_sem.at[s])
                  for s in range(shards)]
    for cp in tok_copies:
        cp.start()

    @pl.when(num_items > 0)
    def _():
        for j in range(up_steps):
            for cp in up_copies(0, j):
                cp.start()
        for j in range(down_steps):
            down_copy(0, j).start()

    def zero(i, c):
        acc[pl.ds(pl.multiple_of(i * 8, 8), 8), :] = jnp.zeros((8, d_model), jnp.float32)
        return c

    lax.fori_loop(0, acc.shape[0] // 8, zero, 0)
    for cp in tok_copies:
        cp.wait()

    def process(m, item, e, p0):
        want = lax.broadcasted_iota(jnp.int32, (m, num_tok), 0) + p0
        onehot[:m, :] = jnp.where(want == pos[e], 1.0, 0.0).astype(jnp.bfloat16)
        parts = lax.dot_general(digits[...], onehot[:m, :], (((1,), (1,)), ((), ())), preferred_element_type=jnp.float32)
        idx = parts[0:1] * ID_RADIX + parts[1:2] + (1.0 - parts[2:3]) * num_tok
        idx_v[:, :m] = jnp.broadcast_to(idx.astype(jnp.int32), (8, m))
        idx_copy = pltpu.make_async_copy(idx_v, idx_s, idx_sem)
        idx_copy.start()

        def dispatch(nb, c):
            cols = pl.ds(pl.multiple_of(nb * OUT_BLOCK, OUT_BLOCK), OUT_BLOCK)
            x[:m, cols] = jnp.dot(onehot[:m, :], tok[:, cols], preferred_element_type=jnp.float32).astype(jnp.bfloat16)
            return c

        lax.fori_loop(0, d_model // OUT_BLOCK, dispatch, 0)

        def up(j, c):
            for cp in up_copies(item, j):
                cp.wait()
            a = jnp.dot(x[:m, :], wg[j], preferred_element_type=jnp.float32)
            u = jnp.dot(x[:m, :], wu[j], preferred_element_type=jnp.float32)
            h[:m, pl.ds(pl.multiple_of(j * FF_BLOCK, FF_BLOCK), FF_BLOCK)] = (jax.nn.silu(a) * u).astype(jnp.bfloat16)

            @pl.when(item + 1 < num_items)
            def _():
                for cp in up_copies(item + 1, j):
                    cp.start()

            return c

        lax.fori_loop(0, up_steps, up, 0)

        def down(j, c):
            down_copy(item, j).wait()
            cols = pl.ds(pl.multiple_of(j * OUT_BLOCK, OUT_BLOCK), OUT_BLOCK)
            o[:m, cols] = jnp.dot(h[:m, :], wd[j], preferred_element_type=jnp.float32)

            @pl.when(item + 1 < num_items)
            def _():
                down_copy(item + 1, j).start()

            return c

        lax.fori_loop(0, down_steps, down, 0)
        idx_copy.wait()

    def scatter(e, rows):
        width = 640

        def eight(i, c):
            base = pl.multiple_of(i * 8, 8)
            for half in range(2):
                t = [idx_s[0, base + half * 4 + k] for k in range(4)]
                g = [gate[e * num_tok + t[k]] for k in range(4)]
                for cb in range(d_model // width):
                    cols = slice(cb * width, (cb + 1) * width)
                    new = [acc[pl.ds(t[k], 1), cols] + o[pl.ds(base + half * 4 + k, 1), cols] * g[k] for k in range(4)]
                    for k in range(4):
                        acc[pl.ds(t[k], 1), cols] = new[k]
            return c

        lax.fori_loop(0, (rows + 7) // 8, eight, 0)

    def item_body(item, c):
        e, p0, rows = meta[item], meta[MAX_ITEMS + item], meta[2 * MAX_ITEMS + item]
        low = 0
        for m in row_sizes:
            @pl.when((rows > low) & (rows <= m))
            def _():
                process(m, item, e, p0)

            low = m
        scatter(e, rows)
        return c

    lax.fori_loop(0, num_items, item_body, 0)
    out_copies = []
    for s in range(shards // 2):
        dst = pl.ds(s * tc, tc)
        mine = pl.ds(pl.multiple_of((2 * s + parity) * tc, tc), tc)
        other = pl.ds(pl.multiple_of((2 * s + 1 - parity) * tc, tc), tc)
        out_copies.append(pltpu.make_async_copy(acc.at[other, :], send_hbm.at[dst, :], out_sem.at[s, 0]))
        out_copies.append(pltpu.make_async_copy(acc.at[mine, :], keep_hbm.at[dst, :], out_sem.at[s, 1]))
    for cp in out_copies:
        cp.start()
    for cp in out_copies:
        cp.wait()


def expert_block(row0, units, meta, gate, pos, digits, tok, w_gate, w_up, w_down):
    shards, _, d_model = tok.shape
    num_tok = shards * units * UNIT
    num_local, _, ff_dim = w_gate.shape
    smem = pl.BlockSpec(memory_space=pltpu.SMEM)
    vmem = pl.BlockSpec(memory_space=pltpu.VMEM)
    anym = pl.BlockSpec(memory_space=pl.ANY)
    rows = num_tok * 3 // 4
    half = jax.ShapeDtypeStruct((num_tok // 2, d_model), jnp.float32)
    up_steps, down_steps = ff_dim // FF_BLOCK, d_model // OUT_BLOCK

    def body(*refs):
        expert_kernel(row0, ROW_SIZES[units], *refs)

    return pl.pallas_call(
        body,
        out_shape=(half, half),
        in_specs=[smem, smem, vmem, vmem, anym, anym, anym, anym],
        out_specs=(anym, anym),
        scratch_shapes=[
            pltpu.VMEM((num_tok, d_model), jnp.bfloat16),
            pltpu.VMEM((num_tok + 8, d_model), jnp.float32),
            pltpu.VMEM((up_steps, d_model, FF_BLOCK), jnp.bfloat16),
            pltpu.VMEM((up_steps, d_model, FF_BLOCK), jnp.bfloat16),
            pltpu.VMEM((down_steps, ff_dim, OUT_BLOCK), jnp.bfloat16),
            pltpu.VMEM((MAX_ROWS, num_tok), jnp.bfloat16),
            pltpu.VMEM((MAX_ROWS, d_model), jnp.bfloat16),
            pltpu.VMEM((MAX_ROWS, ff_dim), jnp.bfloat16),
            pltpu.VMEM((MAX_ROWS, d_model), jnp.float32),
            pltpu.VMEM((8, MAX_ROWS), jnp.int32),
            pltpu.SMEM((8, MAX_ROWS), jnp.int32),
            pltpu.SemaphoreType.DMA((up_steps, 2)),
            pltpu.SemaphoreType.DMA((down_steps,)),
            pltpu.SemaphoreType.DMA((shards,)),
            pltpu.SemaphoreType.DMA,
            pltpu.SemaphoreType.DMA((shards // 2, 2)),
        ],
        compiler_params=pltpu.CompilerParams(vmem_limit_bytes=67_000_000),
        cost_estimate=pl.CostEstimate(flops=rows * 6 * d_model * ff_dim * 2, transcendentals=rows * ff_dim,
                                      bytes_accessed=num_local * 6 * d_model * ff_dim + num_tok * d_model * 6),
        name='expert_block',
    )(meta, gate, pos, digits, tok, w_gate, w_up, w_down)


def pair_kernel(keep, send, out, mine, theirs, send_sem, recv_sem, keep_sem, out_sem):
    me = lax.axis_index('ep')
    other = me + 1 - 2 * lax.rem(me, 2)
    barrier = pltpu.get_barrier_semaphore()
    pl.semaphore_signal(barrier, inc=1, device_id={'ep': other}, device_id_type=pl.DeviceIdType.MESH)
    pl.semaphore_wait(barrier, 1)
    size = keep.shape[0] // PIECES
    remote, local, done = [], [], []
    for p in range(PIECES):
        rows = pl.ds(p * size, size)
        remote.append(pltpu.make_async_remote_copy(
            src_ref=send.at[rows, :], dst_ref=theirs.at[rows, :], send_sem=send_sem.at[p], recv_sem=recv_sem.at[p],
            device_id={'ep': other}, device_id_type=pl.DeviceIdType.MESH))
        local.append(pltpu.make_async_copy(keep.at[rows, :], mine.at[rows, :], keep_sem.at[p]))
        done.append(pltpu.make_async_copy(mine.at[rows, :], out.at[rows, :], out_sem.at[p]))
    for p in range(PIECES):
        remote[p].start()
        local[p].start()
    for p in range(PIECES):
        local[p].wait()
        remote[p].wait_recv()

        def add(i, c, p=p):
            at = pl.ds(pl.multiple_of(p * size + i * 8, 8), 8)
            mine[at, :] = mine[at, :] + theirs[at, :]
            return c

        lax.fori_loop(0, size // 8, add, 0)
        done[p].start()
    for p in range(PIECES):
        remote[p].wait_send()
        done[p].wait()


def pair_sum(keep, send, call_id):
    rows, d_model = keep.shape
    anym = pl.BlockSpec(memory_space=pl.ANY)
    return pl.pallas_call(
        pair_kernel,
        out_shape=jax.ShapeDtypeStruct((rows, d_model), jnp.float32),
        in_specs=[anym, anym],
        out_specs=anym,
        scratch_shapes=[
            pltpu.VMEM((rows, d_model), jnp.float32),
            pltpu.VMEM((rows, d_model), jnp.float32),
            pltpu.SemaphoreType.DMA((PIECES,)),
            pltpu.SemaphoreType.DMA((PIECES,)),
            pltpu.SemaphoreType.DMA((PIECES,)),
            pltpu.SemaphoreType.DMA((PIECES,)),
        ],
        compiler_params=pltpu.CompilerParams(collective_id=call_id, has_side_effects=True, vmem_limit_bytes=67_000_000),
        cost_estimate=pl.CostEstimate(flops=rows * d_model * 4000, transcendentals=0, bytes_accessed=rows * d_model * 16),
        name='pair_sum',
    )(keep, send)


def routing_tables(expert_ids, gate_wts, slot_ids, my_rank, num_local, group_size):
    tok_dev, top_k = expert_ids.shape
    units = tok_dev // UNIT
    key = jnp.where(slot_ids >= 0, expert_ids, -1).astype(jnp.float32).T
    packed = lax.all_gather(jnp.concatenate([key, gate_wts.T], axis=0), 'ep')
    packed = packed.reshape(group_size, 2, top_k, units, UNIT).transpose(1, 2, 0, 3, 4)
    local = (my_rank * num_local + jnp.arange(num_local)).astype(jnp.float32)[:, None, None, None, None]
    hit = packed[0][None] == local
    mask = jnp.any(hit, axis=1)
    gate = jnp.sum(jnp.where(hit, packed[1][None], 0.0), axis=1)

    before = (jnp.arange(UNIT)[:, None] < jnp.arange(UNIT)[None, :]).astype(jnp.bfloat16)
    inner = jnp.einsum('erbk,kl->erbl', mask.astype(jnp.bfloat16), before, preferred_element_type=jnp.float32)
    sums = jnp.sum(mask.astype(jnp.float32), axis=3).reshape(num_local, group_size * units)
    chunk_of_unit = [c for c, n in enumerate(CHUNK_UNITS) for _ in range(n)]
    chunk_of = jnp.tile(jnp.array(chunk_of_unit), group_size)
    block = jnp.arange(group_size * units)
    earlier = (block[:, None] < block[None, :]) & (chunk_of[:, None] == chunk_of[None, :])
    outer = jnp.sum(jnp.where(earlier, sums[:, :, None], 0.0), axis=1).reshape(num_local, group_size, units, 1)
    pos = jnp.where(mask, inner + outer, -1.0).astype(jnp.int32)

    chunks = len(CHUNK_UNITS)
    in_chunk = chunk_of[None, :] == jnp.arange(chunks)[:, None]
    count = jnp.sum(jnp.where(in_chunk[:, None, :], sums[None], 0.0), axis=2).astype(jnp.int32)
    passes = (count + MAX_ROWS - 1) // MAX_ROWS
    upto = jnp.arange(num_local)[:, None] <= jnp.arange(num_local)[None, :]
    ends = jnp.sum(jnp.where(upto, passes[:, :, None], 0), axis=1)
    starts = ends - passes
    item = jnp.arange(MAX_ITEMS)
    mine = (starts[:, :, None] <= item) & (item < ends[:, :, None])
    e = jnp.sum(jnp.where(mine, jnp.arange(num_local)[:, None], 0), axis=1)
    p0 = jnp.sum(jnp.where(mine, (item - starts[:, :, None]) * MAX_ROWS, 0), axis=1)
    rows = jnp.minimum(jnp.sum(jnp.where(mine, count[:, :, None], 0), axis=1) - p0, MAX_ROWS)
    extra = jnp.where(item[None, :] == 0, ends[:, -1:], my_rank % 2)
    meta = jnp.concatenate([e, p0, rows, extra], axis=1).astype(jnp.int32)
    tables = []
    unit0 = 0
    for c, n in enumerate(CHUNK_UNITS):
        span = slice(unit0, unit0 + n)
        num_tok = group_size * n * UNIT
        flat_gate = jnp.pad(gate[:, :, span].reshape(num_local * num_tok), (0, 128))
        tables.append((meta[c], flat_gate, pos[:, :, span].reshape(num_local, 1, num_tok)))
        unit0 += n
    return tables


def solution(mesh):
    group_size = mesh.shape['ep']
    row_spec = P(('dp', 'ep'), None)
    expert_spec = P('ep', None, None)
    same_core = [list(range(core, group_size, 2)) for core in range(2)]

    def per_device(tokens, expert_ids, gate_wts, slot_ids, w_gate, w_up, w_down):
        my_rank = lax.axis_index('ep')
        starts = [UNIT * sum(CHUNK_UNITS[:c]) for c in range(len(CHUNK_UNITS) + 1)]
        source = {}
        for members in GATHERS:
            first, last = starts[members[0]], starts[members[-1] + 1]
            whole = lax.all_gather(tokens[first:last], 'ep', axis=0, tiled=False)
            for c in members:
                source[c] = (whole, starts[c] - first)
        tables = routing_tables(expert_ids, gate_wts, slot_ids, my_rank, w_gate.shape[0], group_size)
        outs = []
        last = None
        for c, units in enumerate(CHUNK_UNITS):
            tok, row0 = source[c]
            ids = jnp.arange(group_size * units * UNIT)
            digits = jnp.stack([ids // ID_RADIX, ids % ID_RADIX, jnp.ones_like(ids)] + [jnp.zeros_like(ids)] * 5).astype(jnp.bfloat16)
            meta, gate, pos = tables[c]
            if last is not None:
                meta, last = lax.optimization_barrier((meta, last))
                outs.append(lax.psum_scatter(last, 'ep', scatter_dimension=0, tiled=True, axis_index_groups=same_core))
            keep, send = expert_block(row0, units, meta, gate, pos, digits, tok, w_gate, w_up, w_down)
            last = pair_sum(keep, send, c)
        outs.append(lax.psum_scatter(last, 'ep', scatter_dimension=0, tiled=True, axis_index_groups=same_core))
        return jnp.concatenate([part.astype(jnp.bfloat16) for part in outs], axis=0)

    return jax.shard_map(per_device, mesh=mesh, in_specs=(row_spec, row_spec, row_spec, row_spec, expert_spec, expert_spec, expert_spec), out_specs=row_spec, check_vma=False)
```

```python
import jax
import jax.numpy as jnp
from jax import lax
from jax.experimental import pallas as pl
from jax.experimental.pallas import tpu as pltpu
from jax.sharding import PartitionSpec as P

UNIT = 128
CHUNK_UNITS = (1, 2, 2, 2, 1)
GATHERS = ((0,), (1,), (2, 3, 4))
ROW_SIZES = {1: (160, 320), 2: (128, 256, 288, 320)}
MAX_ROWS = 320
MAX_ITEMS = 32
FF_BLOCK = 512
FF_PART = 256
OUT_BLOCK = 512
LANES = 128
ID_RADIX = 64
PIECES = 8


def expert_kernel(row0, row_sizes, split, meta, gate, pos, digits, tok_hbm, wg_hbm, wu_hbm, wd_hbm, *refs):
    outs, (tok, acc, wg, wu, wd, onehot, x, h, o, idx_v, idx_s, up_sem, down_sem, tok_sem, idx_sem, out_sem) = refs[:1 + split], refs[1 + split:]
    num_tok, d_model = tok.shape
    shards = tok_hbm.shape[0]
    tc = num_tok // shards
    ff_dim = wg_hbm.shape[2]
    up_steps, down_steps = ff_dim // FF_BLOCK, d_model // OUT_BLOCK
    lines = d_model // LANES
    num_items = meta[3 * MAX_ITEMS]
    parity = meta[3 * MAX_ITEMS + 1]

    def up_copies(item, j):
        cols = pl.ds(pl.multiple_of(j * FF_BLOCK, FF_BLOCK), FF_BLOCK)
        e = meta[item]
        return (pltpu.make_async_copy(wg_hbm.at[e, :, cols], wg.at[j], up_sem.at[j, 0]),
                pltpu.make_async_copy(wu_hbm.at[e, :, cols], wu.at[j], up_sem.at[j, 1]))

    def down_copy(item):
        return pltpu.make_async_copy(wd_hbm.at[meta[item]], wd, down_sem)

    tok_copies = [pltpu.make_async_copy(tok_hbm.at[s, pl.ds(row0, tc), :], tok.at[pl.ds(s * tc, tc), :], tok_sem.at[s])
                  for s in range(shards)]
    for cp in tok_copies:
        cp.start()

    @pl.when(num_items > 0)
    def _():
        for j in range(up_steps):
            for cp in up_copies(0, j):
                cp.start()
        down_copy(0).start()

    def zero(i, c):
        acc[pl.ds(pl.multiple_of(i * 160, 8), 160), :] = jnp.zeros((160, LANES), jnp.float32)
        return c

    lax.fori_loop(0, acc.shape[0] // 160, zero, 0)
    for cp in tok_copies:
        cp.wait()

    def process(m, item, e, p0):
        def select(i, c):
            row = pl.multiple_of(i * 32, 32)
            want = lax.broadcasted_iota(jnp.int32, (32, num_tok), 0) + (p0 + row)
            onehot[pl.ds(row, 32), :] = jnp.where(want == pos[e], 1.0, 0.0).astype(jnp.bfloat16)
            return c

        lax.fori_loop(0, m // 32, select, 0)
        parts = lax.dot_general(digits[...], onehot[:m, :], (((1,), (1,)), ((), ())), preferred_element_type=jnp.float32)
        idx = parts[0:1] * ID_RADIX + parts[1:2] + (1.0 - parts[2:3]) * num_tok
        idx_v[:, :m] = jnp.broadcast_to(idx.astype(jnp.int32), (8, m))
        idx_copy = pltpu.make_async_copy(idx_v, idx_s, idx_sem)
        idx_copy.start()

        def dispatch(nb, c):
            cols = pl.ds(pl.multiple_of(nb * OUT_BLOCK, OUT_BLOCK), OUT_BLOCK)
            x[:m, cols] = jnp.dot(onehot[:m, :], tok[:, cols], preferred_element_type=jnp.float32).astype(jnp.bfloat16)
            return c

        lax.fori_loop(0, d_model // OUT_BLOCK, dispatch, 0)

        def up(j, c):
            for cp in up_copies(item, j):
                cp.wait()

            def part(k, c):
                cols = pl.ds(pl.multiple_of(k * FF_PART, FF_PART), FF_PART)
                a = jnp.dot(x[:m, :], wg[j, :, cols], preferred_element_type=jnp.float32)
                u = jnp.dot(x[:m, :], wu[j, :, cols], preferred_element_type=jnp.float32)
                to = pl.ds(pl.multiple_of(j * FF_BLOCK + k * FF_PART, FF_PART), FF_PART)
                h[:m, to] = (jax.nn.silu(a) * u).astype(jnp.bfloat16)
                return c

            lax.fori_loop(0, FF_BLOCK // FF_PART, part, 0)

            @pl.when(item + 1 < num_items)
            def _():
                for cp in up_copies(item + 1, j):
                    cp.start()

            return c

        lax.fori_loop(0, up_steps, up, 0)
        down_copy(item).wait()

        def down(j, c):
            cols = pl.ds(pl.multiple_of(j * OUT_BLOCK, OUT_BLOCK), OUT_BLOCK)
            part = jnp.dot(h[:m, :], wd[:, cols], preferred_element_type=jnp.float32)
            for k in range(OUT_BLOCK // LANES):
                o[pl.ds(j * (OUT_BLOCK // LANES) + k, m, stride=lines), :] = part[:, k * LANES:(k + 1) * LANES]
            return c

        lax.fori_loop(0, down_steps, down, 0)

        @pl.when(item + 1 < num_items)
        def _():
            down_copy(item + 1).start()

        idx_copy.wait()

    def scatter(e, rows):
        spans = [(at, min(8, lines - at)) for at in range(0, lines, 8)]

        def eight(i, c):
            base = i * 8
            for half in range(2):
                t = [idx_s[0, base + half * 4 + k] for k in range(4)]
                g = [gate[e * num_tok + t[k]] for k in range(4)]
                new = [[acc[pl.ds(t[k] * lines + at, n), :] + o[pl.ds((base + half * 4 + k) * lines + at, n), :] * g[k]
                        for at, n in spans] for k in range(4)]
                for k in range(4):
                    for (at, n), value in zip(spans, new[k]):
                        acc[pl.ds(t[k] * lines + at, n), :] = value
            return c

        lax.fori_loop(0, (rows + 7) // 8, eight, 0)

    def item_body(item, c):
        e, p0, rows = meta[item], meta[MAX_ITEMS + item], meta[2 * MAX_ITEMS + item]
        low = 0
        for m in row_sizes:
            @pl.when((rows > low) & (rows <= m))
            def _():
                process(m, item, e, p0)

            low = m
        scatter(e, rows)
        return c

    lax.fori_loop(0, num_items, item_body, 0)
    out_copies = []
    size = tc * lines
    if split:
        for s in range(shards // 2):
            dst = pl.ds(s * size, size)
            mine = pl.ds(pl.multiple_of((2 * s + parity) * size, size), size)
            other = pl.ds(pl.multiple_of((2 * s + 1 - parity) * size, size), size)
            out_copies.append(pltpu.make_async_copy(acc.at[other, :], outs[1].at[dst, :], out_sem.at[s, 0]))
            out_copies.append(pltpu.make_async_copy(acc.at[mine, :], outs[0].at[dst, :], out_sem.at[s, 1]))
    else:
        out_copies.append(pltpu.make_async_copy(acc.at[pl.ds(0, shards * size), :], outs[0], out_sem.at[0, 0]))
    for cp in out_copies:
        cp.start()
    for cp in out_copies:
        cp.wait()


def expert_block(row0, units, split, meta, gate, pos, digits, tok, w_gate, w_up, w_down):
    shards, _, d_model = tok.shape
    num_tok = shards * units * UNIT
    num_local, _, ff_dim = w_gate.shape
    smem = pl.BlockSpec(memory_space=pltpu.SMEM)
    vmem = pl.BlockSpec(memory_space=pltpu.VMEM)
    anym = pl.BlockSpec(memory_space=pl.ANY)
    rows = num_tok * 3 // 4
    lines = d_model // LANES
    out = jax.ShapeDtypeStruct((num_tok // (1 + split) * lines, LANES), jnp.float32)
    up_steps = ff_dim // FF_BLOCK

    def body(*refs):
        expert_kernel(row0, ROW_SIZES[units], split, *refs)

    return pl.pallas_call(
        body,
        out_shape=(out,) * (1 + split),
        in_specs=[smem, smem, vmem, vmem, anym, anym, anym, anym],
        out_specs=(anym,) * (1 + split),
        scratch_shapes=[
            pltpu.VMEM((num_tok, d_model), jnp.bfloat16),
            pltpu.VMEM(((num_tok + 8) * lines, LANES), jnp.float32),
            pltpu.VMEM((up_steps, d_model, FF_BLOCK), jnp.bfloat16),
            pltpu.VMEM((up_steps, d_model, FF_BLOCK), jnp.bfloat16),
            pltpu.VMEM((ff_dim, d_model), jnp.bfloat16),
            pltpu.VMEM((MAX_ROWS, num_tok), jnp.bfloat16),
            pltpu.VMEM((MAX_ROWS, d_model), jnp.bfloat16),
            pltpu.VMEM((MAX_ROWS, ff_dim), jnp.bfloat16),
            pltpu.VMEM((MAX_ROWS * lines, LANES), jnp.float32),
            pltpu.VMEM((8, MAX_ROWS), jnp.int32),
            pltpu.SMEM((8, MAX_ROWS), jnp.int32),
            pltpu.SemaphoreType.DMA((up_steps, 2)),
            pltpu.SemaphoreType.DMA,
            pltpu.SemaphoreType.DMA((shards,)),
            pltpu.SemaphoreType.DMA,
            pltpu.SemaphoreType.DMA((shards // 2, 2)),
        ],
        compiler_params=pltpu.CompilerParams(vmem_limit_bytes=67_000_000),
        cost_estimate=pl.CostEstimate(flops=rows * 6 * d_model * ff_dim * 2, transcendentals=rows * ff_dim,
                                      bytes_accessed=num_local * 6 * d_model * ff_dim + num_tok * d_model * 6),
        name='expert_block',
    )(meta, gate, pos, digits, tok, w_gate, w_up, w_down)


def pair_kernel(keep, send, out, mine, theirs, send_sem, recv_sem, keep_sem, out_sem):
    me = lax.axis_index('ep')
    other = me + 1 - 2 * lax.rem(me, 2)
    barrier = pltpu.get_barrier_semaphore()
    pl.semaphore_signal(barrier, inc=1, device_id={'ep': other}, device_id_type=pl.DeviceIdType.MESH)
    pl.semaphore_wait(barrier, 1)
    size = keep.shape[0] // PIECES
    remote, local, done = [], [], []
    for p in range(PIECES):
        rows = pl.ds(p * size, size)
        remote.append(pltpu.make_async_remote_copy(
            src_ref=send.at[rows, :], dst_ref=theirs.at[rows, :], send_sem=send_sem.at[p], recv_sem=recv_sem.at[p],
            device_id={'ep': other}, device_id_type=pl.DeviceIdType.MESH))
        local.append(pltpu.make_async_copy(keep.at[rows, :], mine.at[rows, :], keep_sem.at[p]))
        done.append(pltpu.make_async_copy(mine.at[rows, :], out.at[rows, :], out_sem.at[p]))
    for p in range(PIECES):
        remote[p].start()
        local[p].start()
    for p in range(PIECES):
        local[p].wait()
        remote[p].wait_recv()

        def add(i, c, p=p):
            at = pl.ds(pl.multiple_of(p * size + i * 160, 8), 160)
            mine[at, :] = mine[at, :] + theirs[at, :]
            return c

        lax.fori_loop(0, size // 160, add, 0)
        done[p].start()
    for p in range(PIECES):
        remote[p].wait_send()
        done[p].wait()


def pair_sum(keep, send, call_id):
    rows, d_model = keep.shape
    anym = pl.BlockSpec(memory_space=pl.ANY)
    return pl.pallas_call(
        pair_kernel,
        out_shape=jax.ShapeDtypeStruct((rows, d_model), jnp.float32),
        in_specs=[anym, anym],
        out_specs=anym,
        scratch_shapes=[
            pltpu.VMEM((rows, d_model), jnp.float32),
            pltpu.VMEM((rows, d_model), jnp.float32),
            pltpu.SemaphoreType.DMA((PIECES,)),
            pltpu.SemaphoreType.DMA((PIECES,)),
            pltpu.SemaphoreType.DMA((PIECES,)),
            pltpu.SemaphoreType.DMA((PIECES,)),
        ],
        compiler_params=pltpu.CompilerParams(collective_id=call_id, has_side_effects=True, vmem_limit_bytes=67_000_000),
        cost_estimate=pl.CostEstimate(flops=rows * d_model * 4000, transcendentals=0, bytes_accessed=rows * d_model * 16),
        name='pair_sum',
    )(keep, send)


def routing_tables(expert_ids, gate_wts, slot_ids, my_rank, num_local, group_size):
    tok_dev, top_k = expert_ids.shape
    units = tok_dev // UNIT
    key = jnp.where(slot_ids >= 0, expert_ids, -1).astype(jnp.float32).T
    packed = lax.all_gather(jnp.concatenate([key, gate_wts.T], axis=0), 'ep')
    packed = packed.reshape(group_size, 2, top_k, units, UNIT).transpose(1, 2, 0, 3, 4)
    local = (my_rank * num_local + jnp.arange(num_local)).astype(jnp.float32)[:, None, None, None, None]
    hit = packed[0][None] == local
    mask = jnp.any(hit, axis=1)
    gate = jnp.sum(jnp.where(hit, packed[1][None], 0.0), axis=1)

    before = (jnp.arange(UNIT)[:, None] < jnp.arange(UNIT)[None, :]).astype(jnp.bfloat16)
    inner = jnp.einsum('erbk,kl->erbl', mask.astype(jnp.bfloat16), before, preferred_element_type=jnp.float32)
    sums = jnp.sum(mask.astype(jnp.float32), axis=3).reshape(num_local, group_size * units)
    chunk_of_unit = [c for c, n in enumerate(CHUNK_UNITS) for _ in range(n)]
    chunk_of = jnp.tile(jnp.array(chunk_of_unit), group_size)
    block = jnp.arange(group_size * units)
    earlier = (block[:, None] < block[None, :]) & (chunk_of[:, None] == chunk_of[None, :])
    outer = jnp.sum(jnp.where(earlier, sums[:, :, None], 0.0), axis=1).reshape(num_local, group_size, units, 1)
    pos = jnp.where(mask, inner + outer, -1.0).astype(jnp.int32)

    chunks = len(CHUNK_UNITS)
    in_chunk = chunk_of[None, :] == jnp.arange(chunks)[:, None]
    count = jnp.sum(jnp.where(in_chunk[:, None, :], sums[None], 0.0), axis=2).astype(jnp.int32)
    passes = (count + MAX_ROWS - 1) // MAX_ROWS
    upto = jnp.arange(num_local)[:, None] <= jnp.arange(num_local)[None, :]
    ends = jnp.sum(jnp.where(upto, passes[:, :, None], 0), axis=1)
    starts = ends - passes
    item = jnp.arange(MAX_ITEMS)
    mine = (starts[:, :, None] <= item) & (item < ends[:, :, None])
    e = jnp.sum(jnp.where(mine, jnp.arange(num_local)[:, None], 0), axis=1)
    p0 = jnp.sum(jnp.where(mine, (item - starts[:, :, None]) * MAX_ROWS, 0), axis=1)
    rows = jnp.minimum(jnp.sum(jnp.where(mine, count[:, :, None], 0), axis=1) - p0, MAX_ROWS)
    extra = jnp.where(item[None, :] == 0, ends[:, -1:], my_rank % 2)
    meta = jnp.concatenate([e, p0, rows, extra], axis=1).astype(jnp.int32)
    tables = []
    unit0 = 0
    for c, n in enumerate(CHUNK_UNITS):
        span = slice(unit0, unit0 + n)
        num_tok = group_size * n * UNIT
        flat_gate = jnp.pad(gate[:, :, span].reshape(num_local * num_tok), (0, 128))
        tables.append((meta[c], flat_gate, pos[:, :, span].reshape(num_local, 1, num_tok)))
        unit0 += n
    return tables


def solution(mesh):
    group_size = mesh.shape['ep']
    row_spec = P(('dp', 'ep'), None)
    expert_spec = P('ep', None, None)
    same_core = [list(range(core, group_size, 2)) for core in range(2)]

    def layer(tokens, expert_ids, gate_wts, slot_ids, w_gate, w_up, w_down):
        my_rank = lax.axis_index('ep')
        starts = [UNIT * sum(CHUNK_UNITS[:c]) for c in range(len(CHUNK_UNITS) + 1)]
        source = {}
        for members in GATHERS:
            first, last = starts[members[0]], starts[members[-1] + 1]
            whole = lax.all_gather(tokens[first:last], 'ep', axis=0, tiled=False)
            for c in members:
                source[c] = (whole, starts[c] - first)
        tables = routing_tables(expert_ids, gate_wts, slot_ids, my_rank, w_gate.shape[0], group_size)
        outs = []
        last = None

        def reduce(part, c):
            groups = same_core if c > 0 else None
            part = lax.psum_scatter(part, 'ep', scatter_dimension=0, tiled=True, axis_index_groups=groups)
            return part.reshape(-1, tokens.shape[1]).astype(jnp.bfloat16)

        for c, units in enumerate(CHUNK_UNITS):
            tok, row0 = source[c]
            ids = jnp.arange(group_size * units * UNIT)
            digits = jnp.stack([ids // ID_RADIX, ids % ID_RADIX, jnp.ones_like(ids)] + [jnp.zeros_like(ids)] * 5).astype(jnp.bfloat16)
            meta, gate, pos = tables[c]
            if last is not None:
                meta, last = lax.optimization_barrier((meta, last))
                outs.append(reduce(last, c - 1))
            last = expert_block(row0, units, c > 0, meta, gate, pos, digits, tok, w_gate, w_up, w_down)
            last = pair_sum(*last, c) if c > 0 else last[0]
        outs.append(reduce(last, len(CHUNK_UNITS) - 1))
        return jnp.concatenate(outs, axis=0)

    return jax.shard_map(layer, mesh=mesh, in_specs=(row_spec, row_spec, row_spec, row_spec, expert_spec, expert_spec, expert_spec), out_specs=row_spec, check_vma=False)
```

```python
import jax
import jax.numpy as jnp
from jax import lax
from jax.experimental import pallas as pl
from jax.experimental.pallas import tpu as pltpu
from jax.sharding import PartitionSpec as P

UNIT = 128
CHUNK_UNITS = (1, 2, 2, 2, 1)
GATHERS = ((0,), (1,), (2, 3, 4))
ROW_SIZES = {1: (160,), 2: (128, 256, 288, 320)}
MAX_ITEMS = 64
FF_BLOCK = 512
FF_PART = 256
OUT_BLOCK = 512
LANES = 128
ID_RADIX = 64
PIECES = 8


def expert_kernel(row0, row_sizes, meta, gate, pos, digits, tok_hbm, wg_hbm, wu_hbm, wd_hbm, *refs):
    outs, (tok, acc, wg, wu, wd, onehot, x, h, o, idx_v, idx_s, up_sem, down_sem, tok_sem, idx_sem, out_sem) = refs[:2], refs[2:]
    num_tok, d_model = tok.shape
    shards = tok_hbm.shape[0]
    tc = num_tok // shards
    ff_dim = wg_hbm.shape[2]
    up_steps, down_steps = ff_dim // FF_BLOCK, d_model // OUT_BLOCK
    lines = d_model // LANES
    num_items = meta[3 * MAX_ITEMS]
    parity = meta[3 * MAX_ITEMS + 1]

    def up_copies(item, j):
        cols = pl.ds(pl.multiple_of(j * FF_BLOCK, FF_BLOCK), FF_BLOCK)
        e = meta[item]
        return (pltpu.make_async_copy(wg_hbm.at[e, :, cols], wg.at[j], up_sem.at[j, 0]),
                pltpu.make_async_copy(wu_hbm.at[e, :, cols], wu.at[j], up_sem.at[j, 1]))

    def down_copies(item):
        half = ff_dim // 2
        return [pltpu.make_async_copy(wd_hbm.at[meta[item], pl.ds(k * half, half), :], wd.at[pl.ds(k * half, half), :],
                                      down_sem.at[k]) for k in range(2)]

    def start_all(copies):
        for k, cp in enumerate(copies):
            cp.start(priority=k % 2)

    tok_copies = [pltpu.make_async_copy(tok_hbm.at[s, pl.ds(row0, tc), :], tok.at[pl.ds(s * tc, tc), :], tok_sem.at[s])
                  for s in range(shards)]
    start_all(tok_copies)

    @pl.when(num_items > 0)
    def _():
        for j in range(up_steps):
            start_all(up_copies(0, j))
        start_all(down_copies(0))

    def zero(i, c):
        acc[pl.ds(pl.multiple_of(i * 160, 8), 160), :] = jnp.zeros((160, LANES), jnp.float32)
        return c

    lax.fori_loop(0, acc.shape[0] // 160, zero, 0)
    for cp in tok_copies:
        cp.wait()

    def process(m, item, e, p0):
        def select(i, c):
            row = pl.multiple_of(i * 32, 32)
            want = lax.broadcasted_iota(jnp.int32, (32, num_tok), 0) + (p0 + row)
            onehot[pl.ds(row, 32), :] = jnp.where(want == pos[e], 1.0, 0.0).astype(jnp.bfloat16)
            return c

        lax.fori_loop(0, m // 32, select, 0)
        parts = lax.dot_general(digits[...], onehot[:m, :], (((1,), (1,)), ((), ())), preferred_element_type=jnp.float32)
        idx = parts[0:1] * ID_RADIX + parts[1:2] + (1.0 - parts[2:3]) * num_tok
        idx_v[:, :m] = jnp.broadcast_to(idx.astype(jnp.int32), (8, m))
        idx_copy = pltpu.make_async_copy(idx_v, idx_s, idx_sem)
        idx_copy.start()

        def dispatch(nb, c):
            cols = pl.ds(pl.multiple_of(nb * OUT_BLOCK, OUT_BLOCK), OUT_BLOCK)
            x[:m, cols] = jnp.dot(onehot[:m, :], tok[:, cols], preferred_element_type=jnp.float32).astype(jnp.bfloat16)
            return c

        lax.fori_loop(0, d_model // OUT_BLOCK, dispatch, 0)

        def up(j, c):
            for cp in up_copies(item, j):
                cp.wait()

            def part(k, c):
                cols = pl.ds(pl.multiple_of(k * FF_PART, FF_PART), FF_PART)
                a = jnp.dot(x[:m, :], wg[j, :, cols], preferred_element_type=jnp.float32)
                u = jnp.dot(x[:m, :], wu[j, :, cols], preferred_element_type=jnp.float32)
                to = pl.ds(pl.multiple_of(j * FF_BLOCK + k * FF_PART, FF_PART), FF_PART)
                h[:m, to] = (jax.nn.silu(a) * u).astype(jnp.bfloat16)
                return c

            lax.fori_loop(0, FF_BLOCK // FF_PART, part, 0)

            @pl.when(item + 1 < num_items)
            def _():
                start_all(up_copies(item + 1, j))

            return c

        lax.fori_loop(0, up_steps, up, 0)
        for cp in down_copies(item):
            cp.wait()

        def down(j, c):
            cols = pl.ds(pl.multiple_of(j * OUT_BLOCK, OUT_BLOCK), OUT_BLOCK)
            part = jnp.dot(h[:m, :], wd[:, cols], preferred_element_type=jnp.float32)
            for k in range(OUT_BLOCK // LANES):
                o[pl.ds(j * (OUT_BLOCK // LANES) + k, m, stride=lines), :] = part[:, k * LANES:(k + 1) * LANES]
            return c

        lax.fori_loop(0, down_steps, down, 0)

        @pl.when(item + 1 < num_items)
        def _():
            start_all(down_copies(item + 1))

        idx_copy.wait()

    def scatter(e, rows):
        spans = [(at, min(8, lines - at)) for at in range(0, lines, 8)]

        def eight(i, c):
            base = i * 8
            for half in range(2):
                t = [idx_s[0, base + half * 4 + k] for k in range(4)]
                g = [gate[e * num_tok + t[k]] for k in range(4)]
                new = [[acc[pl.ds(t[k] * lines + at, n), :] + o[pl.ds((base + half * 4 + k) * lines + at, n), :] * g[k]
                        for at, n in spans] for k in range(4)]
                for k in range(4):
                    for (at, n), value in zip(spans, new[k]):
                        acc[pl.ds(t[k] * lines + at, n), :] = value
            return c

        lax.fori_loop(0, (rows + 7) // 8, eight, 0)

    def item_body(item, c):
        e, p0, rows = meta[item], meta[MAX_ITEMS + item], meta[2 * MAX_ITEMS + item]
        low = 0
        for m in row_sizes:
            @pl.when((rows > low) & (rows <= m))
            def _():
                process(m, item, e, p0)

            low = m
        scatter(e, rows)
        return c

    lax.fori_loop(0, num_items, item_body, 0)
    out_copies = []
    size = tc * lines
    for s in range(shards // 2):
        dst = pl.ds(s * size, size)
        mine = pl.ds(pl.multiple_of((2 * s + parity) * size, size), size)
        other = pl.ds(pl.multiple_of((2 * s + 1 - parity) * size, size), size)
        out_copies.append(pltpu.make_async_copy(acc.at[other, :], outs[1].at[dst, :], out_sem.at[s, 0]))
        out_copies.append(pltpu.make_async_copy(acc.at[mine, :], outs[0].at[dst, :], out_sem.at[s, 1]))
    start_all(out_copies)
    for cp in out_copies:
        cp.wait()


def expert_block(row0, units, meta, gate, pos, digits, tok, w_gate, w_up, w_down):
    shards, _, d_model = tok.shape
    num_tok = shards * units * UNIT
    num_local, _, ff_dim = w_gate.shape
    smem = pl.BlockSpec(memory_space=pltpu.SMEM)
    vmem = pl.BlockSpec(memory_space=pltpu.VMEM)
    anym = pl.BlockSpec(memory_space=pl.ANY)
    rows = num_tok * 3 // 4
    max_rows = ROW_SIZES[units][-1]
    lines = d_model // LANES
    out = jax.ShapeDtypeStruct((num_tok // 2 * lines, LANES), jnp.float32)
    up_steps = ff_dim // FF_BLOCK

    def body(*refs):
        expert_kernel(row0, ROW_SIZES[units], *refs)

    return pl.pallas_call(
        body,
        out_shape=(out, out),
        in_specs=[smem, smem, vmem, vmem, anym, anym, anym, anym],
        out_specs=(anym, anym),
        scratch_shapes=[
            pltpu.VMEM((num_tok, d_model), jnp.bfloat16),
            pltpu.VMEM(((num_tok + 8) * lines, LANES), jnp.float32),
            pltpu.VMEM((up_steps, d_model, FF_BLOCK), jnp.bfloat16),
            pltpu.VMEM((up_steps, d_model, FF_BLOCK), jnp.bfloat16),
            pltpu.VMEM((ff_dim, d_model), jnp.bfloat16),
            pltpu.VMEM((max_rows, num_tok), jnp.bfloat16),
            pltpu.VMEM((max_rows, d_model), jnp.bfloat16),
            pltpu.VMEM((max_rows, ff_dim), jnp.bfloat16),
            pltpu.VMEM((max_rows * lines, LANES), jnp.float32),
            pltpu.VMEM((8, max_rows), jnp.int32),
            pltpu.SMEM((8, max_rows), jnp.int32),
            pltpu.SemaphoreType.DMA((up_steps, 2)),
            pltpu.SemaphoreType.DMA((2,)),
            pltpu.SemaphoreType.DMA((shards,)),
            pltpu.SemaphoreType.DMA,
            pltpu.SemaphoreType.DMA((shards // 2, 2)),
        ],
        compiler_params=pltpu.CompilerParams(vmem_limit_bytes=67_000_000),
        cost_estimate=pl.CostEstimate(flops=rows * 6 * d_model * ff_dim * 2, transcendentals=rows * ff_dim,
                                      bytes_accessed=num_local * 6 * d_model * ff_dim + num_tok * d_model * 6),
        name='expert_block',
    )(meta, gate, pos, digits, tok, w_gate, w_up, w_down)


def pair_kernel(keep, send, out, mine, theirs, send_sem, recv_sem, keep_sem, out_sem):
    me = lax.axis_index('ep')
    other = me + 1 - 2 * lax.rem(me, 2)
    barrier = pltpu.get_barrier_semaphore()
    pl.semaphore_signal(barrier, inc=1, device_id={'ep': other}, device_id_type=pl.DeviceIdType.MESH)
    pl.semaphore_wait(barrier, 1)
    size = keep.shape[0] // PIECES
    remote, local, done = [], [], []
    for p in range(PIECES):
        rows = pl.ds(p * size, size)
        remote.append(pltpu.make_async_remote_copy(
            src_ref=send.at[rows, :], dst_ref=theirs.at[rows, :], send_sem=send_sem.at[p], recv_sem=recv_sem.at[p],
            device_id={'ep': other}, device_id_type=pl.DeviceIdType.MESH))
        local.append(pltpu.make_async_copy(keep.at[rows, :], mine.at[rows, :], keep_sem.at[p]))
        done.append(pltpu.make_async_copy(mine.at[rows, :], out.at[rows, :], out_sem.at[p]))
    for p in range(PIECES):
        remote[p].start()
        local[p].start()
    for p in range(PIECES):
        local[p].wait()
        remote[p].wait_recv()

        def add(i, c, p=p):
            at = pl.ds(pl.multiple_of(p * size + i * 160, 8), 160)
            mine[at, :] = mine[at, :] + theirs[at, :]
            return c

        lax.fori_loop(0, size // 160, add, 0)
        done[p].start()
    for p in range(PIECES):
        remote[p].wait_send()
        done[p].wait()


def pair_sum(keep, send, call_id):
    rows, d_model = keep.shape
    anym = pl.BlockSpec(memory_space=pl.ANY)
    return pl.pallas_call(
        pair_kernel,
        out_shape=jax.ShapeDtypeStruct((rows, d_model), jnp.float32),
        in_specs=[anym, anym],
        out_specs=anym,
        scratch_shapes=[
            pltpu.VMEM((rows, d_model), jnp.float32),
            pltpu.VMEM((rows, d_model), jnp.float32),
            pltpu.SemaphoreType.DMA((PIECES,)),
            pltpu.SemaphoreType.DMA((PIECES,)),
            pltpu.SemaphoreType.DMA((PIECES,)),
            pltpu.SemaphoreType.DMA((PIECES,)),
        ],
        compiler_params=pltpu.CompilerParams(collective_id=call_id, has_side_effects=True, vmem_limit_bytes=67_000_000),
        cost_estimate=pl.CostEstimate(flops=rows * d_model * 4000, transcendentals=0, bytes_accessed=rows * d_model * 16),
        name='pair_sum',
    )(keep, send)


def routing_tables(expert_ids, gate_wts, slot_ids, my_rank, num_local, group_size):
    tok_dev, top_k = expert_ids.shape
    units = tok_dev // UNIT
    key = jnp.where(slot_ids >= 0, expert_ids, -1).astype(jnp.float32).T
    packed = lax.all_gather(jnp.concatenate([key, gate_wts.T], axis=0), 'ep')
    packed = packed.reshape(group_size, 2, top_k, units, UNIT).transpose(1, 2, 0, 3, 4)
    local = (my_rank * num_local + jnp.arange(num_local)).astype(jnp.float32)[:, None, None, None, None]
    hit = packed[0][None] == local
    mask = jnp.any(hit, axis=1)
    gate = jnp.sum(jnp.where(hit, packed[1][None], 0.0), axis=1)

    before = (jnp.arange(UNIT)[:, None] < jnp.arange(UNIT)[None, :]).astype(jnp.bfloat16)
    inner = jnp.einsum('erbk,kl->erbl', mask.astype(jnp.bfloat16), before, preferred_element_type=jnp.float32)
    sums = jnp.sum(mask.astype(jnp.float32), axis=3).reshape(num_local, group_size * units)
    chunk_of_unit = [c for c, n in enumerate(CHUNK_UNITS) for _ in range(n)]
    chunk_of = jnp.tile(jnp.array(chunk_of_unit), group_size)
    block = jnp.arange(group_size * units)
    earlier = (block[:, None] < block[None, :]) & (chunk_of[:, None] == chunk_of[None, :])
    outer = jnp.sum(jnp.where(earlier, sums[:, :, None], 0.0), axis=1).reshape(num_local, group_size, units, 1)
    pos = jnp.where(mask, inner + outer, -1.0).astype(jnp.int32)

    chunks = len(CHUNK_UNITS)
    in_chunk = chunk_of[None, :] == jnp.arange(chunks)[:, None]
    count = jnp.sum(jnp.where(in_chunk[:, None, :], sums[None], 0.0), axis=2).astype(jnp.int32)
    limit = jnp.array([ROW_SIZES[n][-1] for n in CHUNK_UNITS])[:, None]
    passes = (count + limit - 1) // limit
    upto = jnp.arange(num_local)[:, None] <= jnp.arange(num_local)[None, :]
    ends = jnp.sum(jnp.where(upto, passes[:, :, None], 0), axis=1)
    starts = ends - passes
    item = jnp.arange(MAX_ITEMS)
    mine = (starts[:, :, None] <= item) & (item < ends[:, :, None])
    e = jnp.sum(jnp.where(mine, jnp.arange(num_local)[:, None], 0), axis=1)
    p0 = jnp.sum(jnp.where(mine, (item - starts[:, :, None]) * limit[:, :, None], 0), axis=1)
    rows = jnp.minimum(jnp.sum(jnp.where(mine, count[:, :, None], 0), axis=1) - p0, limit)
    extra = jnp.where(item[None, :] == 0, ends[:, -1:], my_rank % 2)
    meta = jnp.concatenate([e, p0, rows, extra], axis=1).astype(jnp.int32)
    tables = []
    unit0 = 0
    for c, n in enumerate(CHUNK_UNITS):
        span = slice(unit0, unit0 + n)
        num_tok = group_size * n * UNIT
        flat_gate = jnp.pad(gate[:, :, span].reshape(num_local * num_tok), (0, 128))
        tables.append((meta[c], flat_gate, pos[:, :, span].reshape(num_local, 1, num_tok)))
        unit0 += n
    return tables


def solution(mesh):
    group_size = mesh.shape['ep']
    row_spec = P(('dp', 'ep'), None)
    expert_spec = P('ep', None, None)
    same_core = [list(range(core, group_size, 2)) for core in range(2)]

    def layer(tokens, expert_ids, gate_wts, slot_ids, w_gate, w_up, w_down):
        my_rank = lax.axis_index('ep')
        starts = [UNIT * sum(CHUNK_UNITS[:c]) for c in range(len(CHUNK_UNITS) + 1)]
        source = {}
        for members in GATHERS:
            first, last = starts[members[0]], starts[members[-1] + 1]
            whole = lax.all_gather(tokens[first:last], 'ep', axis=0, tiled=False)
            for c in members:
                source[c] = (whole, starts[c] - first)
        tables = routing_tables(expert_ids, gate_wts, slot_ids, my_rank, w_gate.shape[0], group_size)
        outs = []
        last = None

        def reduce(part):
            part = lax.psum_scatter(part, 'ep', scatter_dimension=0, tiled=True, axis_index_groups=same_core)
            return part.reshape(-1, tokens.shape[1]).astype(jnp.bfloat16)

        for c, units in enumerate(CHUNK_UNITS):
            tok, row0 = source[c]
            ids = jnp.arange(group_size * units * UNIT)
            digits = jnp.stack([ids // ID_RADIX, ids % ID_RADIX, jnp.ones_like(ids)] + [jnp.zeros_like(ids)] * 5).astype(jnp.bfloat16)
            meta, gate, pos = tables[c]
            if last is not None:
                meta, last = lax.optimization_barrier((meta, last))
                outs.append(reduce(last))
            last = expert_block(row0, units, meta, gate, pos, digits, tok, w_gate, w_up, w_down)
            last = pair_sum(*last, c)
        outs.append(reduce(last))
        return jnp.concatenate(outs, axis=0)

    return jax.shard_map(layer, mesh=mesh, in_specs=(row_spec, row_spec, row_spec, row_spec, expert_spec, expert_spec, expert_spec), out_specs=row_spec, check_vma=False)
```

```python
import jax
import jax.numpy as jnp
from jax import lax
from jax.experimental import pallas as pl
from jax.experimental.pallas import tpu as pltpu
from jax.sharding import PartitionSpec as P

UNIT = 64
CHUNK_UNITS = (3, 4, 4, 3, 2)
GATHERS = ((0,), (1,), (2, 3, 4))
ROW_SIZES = {2: (160,), 3: (192, 224), 4: (128, 256, 288, 320)}
MAX_ITEMS = 64
FF_BLOCK = 512
FF_PART = 256
OUT_BLOCK = 512
LANES = 128
ID_RADIX = 64
PIECES = 8


def expert_kernel(row0, row_sizes, meta, gate, pos, digits, tok_hbm, wg_hbm, wu_hbm, wd_hbm, *refs):
    outs, (tok, acc, wg, wu, wd, onehot, x, h, o, idx_v, idx_s, up_sem, down_sem, tok_sem, idx_sem, out_sem) = refs[:2], refs[2:]
    num_tok, d_model = tok.shape
    shards = tok_hbm.shape[0]
    tc = num_tok // shards
    ff_dim = wg_hbm.shape[2]
    up_steps, down_steps = ff_dim // FF_BLOCK, d_model // OUT_BLOCK
    lines = d_model // LANES
    num_items = meta[3 * MAX_ITEMS]
    parity = meta[3 * MAX_ITEMS + 1]

    def up_copies(item, j):
        cols = pl.ds(pl.multiple_of(j * FF_BLOCK, FF_BLOCK), FF_BLOCK)
        e = meta[item]
        return (pltpu.make_async_copy(wg_hbm.at[e, :, cols], wg.at[j], up_sem.at[j, 0]),
                pltpu.make_async_copy(wu_hbm.at[e, :, cols], wu.at[j], up_sem.at[j, 1]))

    def down_copies(item):
        half = ff_dim // 2
        return [pltpu.make_async_copy(wd_hbm.at[meta[item], pl.ds(k * half, half), :], wd.at[pl.ds(k * half, half), :],
                                      down_sem.at[k]) for k in range(2)]

    def start_all(copies):
        for cp in copies:
            cp.start()

    tok_copies = [pltpu.make_async_copy(tok_hbm.at[s, pl.ds(row0, tc), :], tok.at[pl.ds(s * tc, tc), :], tok_sem.at[s])
                  for s in range(shards)]
    start_all(tok_copies)

    @pl.when(num_items > 0)
    def _():
        for j in range(up_steps):
            start_all(up_copies(0, j))
        start_all(down_copies(0))

    def zero(i, c):
        acc[pl.ds(pl.multiple_of(i * 160, 8), 160), :] = jnp.zeros((160, LANES), jnp.float32)
        return c

    lax.fori_loop(0, acc.shape[0] // 160, zero, 0)
    for cp in tok_copies:
        cp.wait()

    def process(m, item, e, p0):
        def select(i, c):
            row = pl.multiple_of(i * 32, 32)
            want = lax.broadcasted_iota(jnp.int32, (32, num_tok), 0) + (p0 + row)
            onehot[pl.ds(row, 32), :] = jnp.where(want == pos[e], 1.0, 0.0).astype(jnp.bfloat16)
            return c

        lax.fori_loop(0, m // 32, select, 0)
        parts = lax.dot_general(digits[...], onehot[:m, :], (((1,), (1,)), ((), ())), preferred_element_type=jnp.float32)
        idx = parts[0:1] * ID_RADIX + parts[1:2] + (1.0 - parts[2:3]) * num_tok
        idx_v[:, :m] = jnp.broadcast_to(idx.astype(jnp.int32), (8, m))
        idx_copy = pltpu.make_async_copy(idx_v, idx_s, idx_sem)
        idx_copy.start()

        def dispatch(nb, c):
            cols = pl.ds(pl.multiple_of(nb * OUT_BLOCK, OUT_BLOCK), OUT_BLOCK)
            x[:m, cols] = jnp.dot(onehot[:m, :], tok[:, cols], preferred_element_type=jnp.float32).astype(jnp.bfloat16)
            return c

        lax.fori_loop(0, d_model // OUT_BLOCK, dispatch, 0)

        def up(j, c):
            for cp in up_copies(item, j):
                cp.wait()

            def part(k, c):
                cols = pl.ds(pl.multiple_of(k * FF_PART, FF_PART), FF_PART)
                a = jnp.dot(x[:m, :], wg[j, :, cols], preferred_element_type=jnp.float32)
                u = jnp.dot(x[:m, :], wu[j, :, cols], preferred_element_type=jnp.float32)
                to = pl.ds(pl.multiple_of(j * FF_BLOCK + k * FF_PART, FF_PART), FF_PART)
                h[:m, to] = (jax.nn.silu(a) * u).astype(jnp.bfloat16)
                return c

            lax.fori_loop(0, FF_BLOCK // FF_PART, part, 0)

            @pl.when(item + 1 < num_items)
            def _():
                start_all(up_copies(item + 1, j))

            return c

        lax.fori_loop(0, up_steps, up, 0)
        for cp in down_copies(item):
            cp.wait()

        def down(j, c):
            cols = pl.ds(pl.multiple_of(j * OUT_BLOCK, OUT_BLOCK), OUT_BLOCK)
            part = jnp.dot(h[:m, :], wd[:, cols], preferred_element_type=jnp.float32)
            for k in range(OUT_BLOCK // LANES):
                o[pl.ds(j * (OUT_BLOCK // LANES) + k, m, stride=lines), :] = part[:, k * LANES:(k + 1) * LANES]
            return c

        lax.fori_loop(0, down_steps, down, 0)

        @pl.when(item + 1 < num_items)
        def _():
            start_all(down_copies(item + 1))

        idx_copy.wait()

    def scatter(e, rows):
        spans = [(at, min(8, lines - at)) for at in range(0, lines, 8)]

        def eight(i, c):
            base = i * 8
            for half in range(2):
                t = [idx_s[0, base + half * 4 + k] for k in range(4)]
                g = [gate[e * num_tok + t[k]] for k in range(4)]
                new = [[acc[pl.ds(t[k] * lines + at, n), :] + o[pl.ds((base + half * 4 + k) * lines + at, n), :] * g[k]
                        for at, n in spans] for k in range(4)]
                for k in range(4):
                    for (at, n), value in zip(spans, new[k]):
                        acc[pl.ds(t[k] * lines + at, n), :] = value
            return c

        lax.fori_loop(0, (rows + 7) // 8, eight, 0)

    def item_body(item, c):
        e, p0, rows = meta[item], meta[MAX_ITEMS + item], meta[2 * MAX_ITEMS + item]
        low = 0
        for m in row_sizes:
            @pl.when((rows > low) & (rows <= m))
            def _():
                process(m, item, e, p0)

            low = m
        scatter(e, rows)
        return c

    lax.fori_loop(0, num_items, item_body, 0)
    out_copies = []
    size = tc * lines
    for s in range(shards // 2):
        dst = pl.ds(s * size, size)
        mine = pl.ds(pl.multiple_of((2 * s + parity) * size, size), size)
        other = pl.ds(pl.multiple_of((2 * s + 1 - parity) * size, size), size)
        out_copies.append(pltpu.make_async_copy(acc.at[other, :], outs[1].at[dst, :], out_sem.at[s, 0]))
        out_copies.append(pltpu.make_async_copy(acc.at[mine, :], outs[0].at[dst, :], out_sem.at[s, 1]))
    start_all(out_copies)
    for cp in out_copies:
        cp.wait()


def expert_block(row0, units, meta, gate, pos, digits, tok, w_gate, w_up, w_down):
    shards, _, d_model = tok.shape
    num_tok = shards * units * UNIT
    num_local, _, ff_dim = w_gate.shape
    smem = pl.BlockSpec(memory_space=pltpu.SMEM)
    vmem = pl.BlockSpec(memory_space=pltpu.VMEM)
    anym = pl.BlockSpec(memory_space=pl.ANY)
    rows = num_tok * 3 // 4
    max_rows = ROW_SIZES[units][-1]
    lines = d_model // LANES
    out = jax.ShapeDtypeStruct((num_tok // 2 * lines, LANES), jnp.float32)
    up_steps = ff_dim // FF_BLOCK

    def body(*refs):
        expert_kernel(row0, ROW_SIZES[units], *refs)

    return pl.pallas_call(
        body,
        out_shape=(out, out),
        in_specs=[smem, smem, vmem, vmem, anym, anym, anym, anym],
        out_specs=(anym, anym),
        scratch_shapes=[
            pltpu.VMEM((num_tok, d_model), jnp.bfloat16),
            pltpu.VMEM(((num_tok + 8) * lines, LANES), jnp.float32),
            pltpu.VMEM((up_steps, d_model, FF_BLOCK), jnp.bfloat16),
            pltpu.VMEM((up_steps, d_model, FF_BLOCK), jnp.bfloat16),
            pltpu.VMEM((ff_dim, d_model), jnp.bfloat16),
            pltpu.VMEM((max_rows, num_tok), jnp.bfloat16),
            pltpu.VMEM((max_rows, d_model), jnp.bfloat16),
            pltpu.VMEM((max_rows, ff_dim), jnp.bfloat16),
            pltpu.VMEM((max_rows * lines, LANES), jnp.float32),
            pltpu.VMEM((8, max_rows), jnp.int32),
            pltpu.SMEM((8, max_rows), jnp.int32),
            pltpu.SemaphoreType.DMA((up_steps, 2)),
            pltpu.SemaphoreType.DMA((2,)),
            pltpu.SemaphoreType.DMA((shards,)),
            pltpu.SemaphoreType.DMA,
            pltpu.SemaphoreType.DMA((shards // 2, 2)),
        ],
        compiler_params=pltpu.CompilerParams(vmem_limit_bytes=67_000_000),
        cost_estimate=pl.CostEstimate(flops=rows * 6 * d_model * ff_dim * 2, transcendentals=rows * ff_dim,
                                      bytes_accessed=num_local * 6 * d_model * ff_dim + num_tok * d_model * 6),
        name='expert_block',
    )(meta, gate, pos, digits, tok, w_gate, w_up, w_down)


def pair_kernel(keep, send, out, mine, theirs, send_sem, recv_sem, keep_sem, out_sem):
    me = lax.axis_index('ep')
    other = me + 1 - 2 * lax.rem(me, 2)
    barrier = pltpu.get_barrier_semaphore()
    pl.semaphore_signal(barrier, inc=1, device_id={'ep': other}, device_id_type=pl.DeviceIdType.MESH)
    pl.semaphore_wait(barrier, 1)
    size = keep.shape[0] // PIECES
    remote, local, done = [], [], []
    for p in range(PIECES):
        rows = pl.ds(p * size, size)
        remote.append(pltpu.make_async_remote_copy(
            src_ref=send.at[rows, :], dst_ref=theirs.at[rows, :], send_sem=send_sem.at[p], recv_sem=recv_sem.at[p],
            device_id={'ep': other}, device_id_type=pl.DeviceIdType.MESH))
        local.append(pltpu.make_async_copy(keep.at[rows, :], mine.at[rows, :], keep_sem.at[p]))
        done.append(pltpu.make_async_copy(mine.at[rows, :], out.at[rows, :], out_sem.at[p]))
    for p in range(PIECES):
        remote[p].start()
        local[p].start()
    for p in range(PIECES):
        local[p].wait()
        remote[p].wait_recv()

        def add(i, c, p=p):
            at = pl.ds(pl.multiple_of(p * size + i * 160, 8), 160)
            mine[at, :] = mine[at, :] + theirs[at, :]
            return c

        lax.fori_loop(0, size // 160, add, 0)
        done[p].start()
    for p in range(PIECES):
        remote[p].wait_send()
        done[p].wait()


def pair_sum(keep, send, call_id):
    rows, d_model = keep.shape
    anym = pl.BlockSpec(memory_space=pl.ANY)
    return pl.pallas_call(
        pair_kernel,
        out_shape=jax.ShapeDtypeStruct((rows, d_model), jnp.float32),
        in_specs=[anym, anym],
        out_specs=anym,
        scratch_shapes=[
            pltpu.VMEM((rows, d_model), jnp.float32),
            pltpu.VMEM((rows, d_model), jnp.float32),
            pltpu.SemaphoreType.DMA((PIECES,)),
            pltpu.SemaphoreType.DMA((PIECES,)),
            pltpu.SemaphoreType.DMA((PIECES,)),
            pltpu.SemaphoreType.DMA((PIECES,)),
        ],
        compiler_params=pltpu.CompilerParams(collective_id=call_id, has_side_effects=True, vmem_limit_bytes=67_000_000),
        cost_estimate=pl.CostEstimate(flops=rows * d_model * 4000, transcendentals=0, bytes_accessed=rows * d_model * 16),
        name='pair_sum',
    )(keep, send)


def routing_tables(expert_ids, gate_wts, slot_ids, my_rank, num_local, group_size):
    tok_dev, top_k = expert_ids.shape
    units = tok_dev // UNIT
    key = jnp.where(slot_ids >= 0, expert_ids, -1).astype(jnp.float32).T
    packed = lax.all_gather(jnp.concatenate([key, gate_wts.T], axis=0), 'ep')
    packed = packed.reshape(group_size, 2, top_k, units, UNIT).transpose(1, 2, 0, 3, 4)
    local = (my_rank * num_local + jnp.arange(num_local)).astype(jnp.float32)[:, None, None, None, None]
    hit = packed[0][None] == local
    mask = jnp.any(hit, axis=1)
    gate = jnp.sum(jnp.where(hit, packed[1][None], 0.0), axis=1)

    before = (jnp.arange(UNIT)[:, None] < jnp.arange(UNIT)[None, :]).astype(jnp.bfloat16)
    inner = jnp.einsum('erbk,kl->erbl', mask.astype(jnp.bfloat16), before, preferred_element_type=jnp.float32)
    sums = jnp.sum(mask.astype(jnp.float32), axis=3).reshape(num_local, group_size * units)
    chunk_of_unit = [c for c, n in enumerate(CHUNK_UNITS) for _ in range(n)]
    chunk_of = jnp.tile(jnp.array(chunk_of_unit), group_size)
    block = jnp.arange(group_size * units)
    earlier = (block[:, None] < block[None, :]) & (chunk_of[:, None] == chunk_of[None, :])
    outer = jnp.sum(jnp.where(earlier, sums[:, :, None], 0.0), axis=1).reshape(num_local, group_size, units, 1)
    pos = jnp.where(mask, inner + outer, -1.0).astype(jnp.int32)

    chunks = len(CHUNK_UNITS)
    in_chunk = chunk_of[None, :] == jnp.arange(chunks)[:, None]
    count = jnp.sum(jnp.where(in_chunk[:, None, :], sums[None], 0.0), axis=2).astype(jnp.int32)
    limit = jnp.array([ROW_SIZES[n][-1] for n in CHUNK_UNITS])[:, None]
    passes = (count + limit - 1) // limit
    upto = jnp.arange(num_local)[:, None] <= jnp.arange(num_local)[None, :]
    ends = jnp.sum(jnp.where(upto, passes[:, :, None], 0), axis=1)
    starts = ends - passes
    item = jnp.arange(MAX_ITEMS)
    mine = (starts[:, :, None] <= item) & (item < ends[:, :, None])
    e = jnp.sum(jnp.where(mine, jnp.arange(num_local)[:, None], 0), axis=1)
    p0 = jnp.sum(jnp.where(mine, (item - starts[:, :, None]) * limit[:, :, None], 0), axis=1)
    rows = jnp.minimum(jnp.sum(jnp.where(mine, count[:, :, None], 0), axis=1) - p0, limit)
    extra = jnp.where(item[None, :] == 0, ends[:, -1:], my_rank % 2)
    meta = jnp.concatenate([e, p0, rows, extra], axis=1).astype(jnp.int32)
    tables = []
    unit0 = 0
    for c, n in enumerate(CHUNK_UNITS):
        span = slice(unit0, unit0 + n)
        num_tok = group_size * n * UNIT
        flat_gate = jnp.pad(gate[:, :, span].reshape(num_local * num_tok), (0, 128))
        tables.append((meta[c], flat_gate, pos[:, :, span].reshape(num_local, 1, num_tok)))
        unit0 += n
    return tables


def solution(mesh):
    group_size = mesh.shape['ep']
    row_spec = P(('dp', 'ep'), None)
    expert_spec = P('ep', None, None)
    same_core = [list(range(core, group_size, 2)) for core in range(2)]

    def layer(tokens, expert_ids, gate_wts, slot_ids, w_gate, w_up, w_down):
        my_rank = lax.axis_index('ep')
        starts = [UNIT * sum(CHUNK_UNITS[:c]) for c in range(len(CHUNK_UNITS) + 1)]
        source = {}
        for members in GATHERS:
            first, last = starts[members[0]], starts[members[-1] + 1]
            whole = lax.all_gather(tokens[first:last], 'ep', axis=0, tiled=False)
            for c in members:
                source[c] = (whole, starts[c] - first)
        tables = routing_tables(expert_ids, gate_wts, slot_ids, my_rank, w_gate.shape[0], group_size)
        outs = []
        last = None

        def reduce(part):
            part = lax.psum_scatter(part, 'ep', scatter_dimension=0, tiled=True, axis_index_groups=same_core)
            return part.reshape(-1, tokens.shape[1]).astype(jnp.bfloat16)

        for c, units in enumerate(CHUNK_UNITS):
            tok, row0 = source[c]
            ids = jnp.arange(group_size * units * UNIT)
            digits = jnp.stack([ids // ID_RADIX, ids % ID_RADIX, jnp.ones_like(ids)] + [jnp.zeros_like(ids)] * 5).astype(jnp.bfloat16)
            meta, gate, pos = tables[c]
            if last is not None:
                meta, last = lax.optimization_barrier((meta, last))
                outs.append(reduce(last))
            last = expert_block(row0, units, meta, gate, pos, digits, tok, w_gate, w_up, w_down)
            last = pair_sum(*last, c)
        outs.append(reduce(last))
        return jnp.concatenate(outs, axis=0)

    return jax.shard_map(layer, mesh=mesh, in_specs=(row_spec, row_spec, row_spec, row_spec, expert_spec, expert_spec, expert_spec), out_specs=row_spec, check_vma=False)
```

```python
import jax
import jax.numpy as jnp
from jax import lax
from jax.experimental import pallas as pl
from jax.experimental.pallas import tpu as pltpu
from jax.sharding import PartitionSpec as P

UNIT = 128
CHUNK_UNITS = (1, 2, 2, 2, 1)
GATHERS = ((0,), (1,), (2, 3, 4))
ROW_SIZES = {1: (160,), 2: (128, 256, 288, 320)}
MAX_ITEMS = 64
FF_BLOCK = 512
FF_PART = 256
OUT_BLOCK = 512
LANES = 128
ID_RADIX = 64
WINDOW = 10
PIECES = 8


def expert_kernel(row0, row_sizes, meta, gate, pos, digits, tok_hbm, wg_hbm, wu_hbm, wd_hbm, *refs):
    outs, (tok, acc, wg, wu, wd, onehot, x, h, o, idx_v, idx_s, up_sem, down_sem, tok_sem, idx_sem, out_sem) = refs[:2], refs[2:]
    num_tok, d_model = tok.shape
    shards = tok_hbm.shape[0]
    tc = num_tok // shards
    ff_dim = wg_hbm.shape[2]
    up_steps, down_steps = ff_dim // FF_BLOCK, d_model // OUT_BLOCK
    lines = d_model // LANES
    num_items = meta[3 * MAX_ITEMS]
    parity = meta[3 * MAX_ITEMS + 1]

    def up_copies(item, j):
        cols = pl.ds(pl.multiple_of(j * FF_BLOCK, FF_BLOCK), FF_BLOCK)
        e = meta[item]
        return (pltpu.make_async_copy(wg_hbm.at[e, :, cols], wg.at[j], up_sem.at[j, 0]),
                pltpu.make_async_copy(wu_hbm.at[e, :, cols], wu.at[j], up_sem.at[j, 1]))

    def down_copies(item):
        half = ff_dim // 2
        return [pltpu.make_async_copy(wd_hbm.at[meta[item], pl.ds(k * half, half), :], wd.at[pl.ds(k * half, half), :],
                                      down_sem.at[k]) for k in range(2)]

    def start_all(copies):
        for cp in copies:
            cp.start()

    tok_copies = [pltpu.make_async_copy(tok_hbm.at[s, pl.ds(row0, tc), :], tok.at[pl.ds(s * tc, tc), :], tok_sem.at[s])
                  for s in range(shards)]
    start_all(tok_copies)

    @pl.when(num_items > 0)
    def _():
        for j in range(up_steps):
            start_all(up_copies(0, j))
        start_all(down_copies(0))

    def zero(i, c):
        acc[pl.ds(pl.multiple_of(i * 160, 8), 160), :] = jnp.zeros((160, LANES), jnp.float32)
        return c

    lax.fori_loop(0, acc.shape[0] // 160, zero, 0)
    for cp in tok_copies:
        cp.wait()

    max_rows = row_sizes[-1]
    blocks = num_tok // UNIT

    def block_of(e, p):
        found = -1
        for k in range(blocks):
            found = found + jnp.where(meta[4 * MAX_ITEMS + e * blocks + k] <= p, 1, 0)
        return found

    def dispatch(rows, e, row0, p0, half, first, width):
        start = pl.multiple_of(first * UNIT, UNIT)

        def select(i, c):
            row = pl.multiple_of(i * 16, 16)
            want = lax.broadcasted_iota(jnp.int32, (16, width), 0) + (p0 + row)
            here = pos[e, :, pl.ds(start, width)]
            onehot[pl.ds(row, 16), :width] = jnp.where(want == here, 1.0, 0.0).astype(jnp.bfloat16)
            return c

        lax.fori_loop(0, rows // 16, select, 0)
        parts = lax.dot_general(digits[:, :width], onehot[:rows, :width], (((1,), (1,)), ((), ())), preferred_element_type=jnp.float32)
        here = parts[0:1] * ID_RADIX + parts[1:2] + (parts[2:3] * start.astype(jnp.float32) + (1.0 - parts[2:3]) * num_tok)
        idx_v[pl.ds(pl.multiple_of(half * 8, 8), 8), :rows] = jnp.broadcast_to(here.astype(jnp.int32), (8, rows))

        def columns(nb, c):
            cols = pl.ds(pl.multiple_of(nb * OUT_BLOCK, OUT_BLOCK), OUT_BLOCK)
            x[pl.ds(pl.multiple_of(row0, 16), rows), cols] = jnp.dot(
                onehot[:rows, :width], tok[pl.ds(start, width), cols], preferred_element_type=jnp.float32).astype(jnp.bfloat16)
            return c

        lax.fori_loop(0, d_model // OUT_BLOCK, columns, 0)

    idx_copy = pltpu.make_async_copy(idx_v, idx_s, idx_sem)
    zero_block = jnp.int32(0)

    def process(m, item):
        def up(j, c):
            for cp in up_copies(item, j):
                cp.wait()

            def part(k, c):
                cols = pl.ds(pl.multiple_of(k * FF_PART, FF_PART), FF_PART)
                a = jnp.dot(x[:m, :], wg[j, :, cols], preferred_element_type=jnp.float32)
                u = jnp.dot(x[:m, :], wu[j, :, cols], preferred_element_type=jnp.float32)
                to = pl.ds(pl.multiple_of(j * FF_BLOCK + k * FF_PART, FF_PART), FF_PART)
                h[:m, to] = (jax.nn.silu(a) * u).astype(jnp.bfloat16)
                return c

            lax.fori_loop(0, FF_BLOCK // FF_PART, part, 0)

            @pl.when(item + 1 < num_items)
            def _():
                start_all(up_copies(item + 1, j))

            return c

        lax.fori_loop(0, up_steps, up, 0)
        for cp in down_copies(item):
            cp.wait()

        def down(j, c):
            cols = pl.ds(pl.multiple_of(j * OUT_BLOCK, OUT_BLOCK), OUT_BLOCK)
            part = jnp.dot(h[:m, :], wd[:, cols], preferred_element_type=jnp.float32)
            for k in range(OUT_BLOCK // LANES):
                o[pl.ds(j * (OUT_BLOCK // LANES) + k, m, stride=lines), :] = part[:, k * LANES:(k + 1) * LANES]
            return c

        lax.fori_loop(0, down_steps, down, 0)

        @pl.when(item + 1 < num_items)
        def _():
            start_all(down_copies(item + 1))

    def scatter(e, rows, half_rows):
        spans = [(at, min(8, lines - at)) for at in range(0, lines, 8)]

        def eight(i, c):
            base = i * 8
            upper = jnp.where(base >= half_rows, 1, 0)
            at0 = base - upper * half_rows
            for half in range(2):
                t = [idx_s[upper * 8, at0 + half * 4 + k] for k in range(4)]
                g = [gate[e * num_tok + t[k]] for k in range(4)]
                new = [[acc[pl.ds(t[k] * lines + at, n), :] + o[pl.ds((base + half * 4 + k) * lines + at, n), :] * g[k]
                        for at, n in spans] for k in range(4)]
                for k in range(4):
                    for (at, n), value in zip(spans, new[k]):
                        acc[pl.ds(t[k] * lines + at, n), :] = value
            return c

        lax.fori_loop(0, (rows + 7) // 8, eight, 0)

    def item_body(item, c):
        e, p0, rows = meta[item], meta[MAX_ITEMS + item], meta[2 * MAX_ITEMS + item]
        half_rows = max_rows
        windowed = False
        starts = (zero_block, zero_block)
        low = 0
        if blocks > WINDOW:
            for m in row_sizes[1:]:
                half_rows = jnp.where(rows <= m, jnp.minimum(half_rows, m // 2), half_rows)
            fits = rows > row_sizes[0]
            starts = []
            for half in range(2):
                begin = p0 + half * half_rows
                end = jnp.minimum(begin + half_rows, p0 + rows) - 1
                first = jnp.minimum(block_of(e, begin), blocks - WINDOW)
                fits = fits & (block_of(e, end) < first + WINDOW)
                starts.append(first)
            windowed = fits
            half_rows = jnp.where(fits, half_rows, max_rows)
            for m in row_sizes[1:]:
                @pl.when(windowed & (half_rows == m // 2))
                def _():
                    def half_step(half, c):
                        first = jnp.where(half == 0, starts[0], starts[1])
                        dispatch(m // 2, e, half * (m // 2), p0 + half * (m // 2), half, first, WINDOW * UNIT)
                        return c

                    lax.fori_loop(0, 2, half_step, 0)

            @pl.when(rows <= row_sizes[0])
            def _():
                dispatch(row_sizes[0], e, 0, p0, 0, zero_block, num_tok)

            @pl.when((rows > row_sizes[0]) & jnp.logical_not(windowed))
            def _():
                dispatch(max_rows, e, 0, p0, 0, zero_block, num_tok)
        else:
            dispatch(max_rows, e, 0, p0, 0, zero_block, num_tok)
        idx_copy.start()
        for m in row_sizes:
            @pl.when((rows > low) & (rows <= m))
            def _():
                process(m, item)

            low = m
        idx_copy.wait()
        scatter(e, rows, half_rows)
        return c

    lax.fori_loop(0, num_items, item_body, 0)
    out_copies = []
    size = tc * lines
    for s in range(shards // 2):
        dst = pl.ds(s * size, size)
        mine = pl.ds(pl.multiple_of((2 * s + parity) * size, size), size)
        other = pl.ds(pl.multiple_of((2 * s + 1 - parity) * size, size), size)
        out_copies.append(pltpu.make_async_copy(acc.at[other, :], outs[1].at[dst, :], out_sem.at[s, 0]))
        out_copies.append(pltpu.make_async_copy(acc.at[mine, :], outs[0].at[dst, :], out_sem.at[s, 1]))
    start_all(out_copies)
    for cp in out_copies:
        cp.wait()


def expert_block(row0, units, meta, gate, pos, digits, tok, w_gate, w_up, w_down):
    shards, _, d_model = tok.shape
    num_tok = shards * units * UNIT
    num_local, _, ff_dim = w_gate.shape
    smem = pl.BlockSpec(memory_space=pltpu.SMEM)
    vmem = pl.BlockSpec(memory_space=pltpu.VMEM)
    anym = pl.BlockSpec(memory_space=pl.ANY)
    rows = num_tok * 3 // 4
    max_rows = ROW_SIZES[units][-1]
    lines = d_model // LANES
    out = jax.ShapeDtypeStruct((num_tok // 2 * lines, LANES), jnp.float32)
    up_steps = ff_dim // FF_BLOCK

    def body(*refs):
        expert_kernel(row0, ROW_SIZES[units], *refs)

    return pl.pallas_call(
        body,
        out_shape=(out, out),
        in_specs=[smem, smem, vmem, vmem, anym, anym, anym, anym],
        out_specs=(anym, anym),
        scratch_shapes=[
            pltpu.VMEM((num_tok, d_model), jnp.bfloat16),
            pltpu.VMEM(((num_tok + 8) * lines, LANES), jnp.float32),
            pltpu.VMEM((up_steps, d_model, FF_BLOCK), jnp.bfloat16),
            pltpu.VMEM((up_steps, d_model, FF_BLOCK), jnp.bfloat16),
            pltpu.VMEM((ff_dim, d_model), jnp.bfloat16),
            pltpu.VMEM((max_rows, num_tok), jnp.bfloat16),
            pltpu.VMEM((max_rows, d_model), jnp.bfloat16),
            pltpu.VMEM((max_rows, ff_dim), jnp.bfloat16),
            pltpu.VMEM((max_rows * lines, LANES), jnp.float32),
            pltpu.VMEM((16, max_rows), jnp.int32),
            pltpu.SMEM((16, max_rows), jnp.int32),
            pltpu.SemaphoreType.DMA((up_steps, 2)),
            pltpu.SemaphoreType.DMA((2,)),
            pltpu.SemaphoreType.DMA((shards,)),
            pltpu.SemaphoreType.DMA,
            pltpu.SemaphoreType.DMA((shards // 2, 2)),
        ],
        compiler_params=pltpu.CompilerParams(vmem_limit_bytes=67_000_000),
        cost_estimate=pl.CostEstimate(flops=rows * 6 * d_model * ff_dim * 2, transcendentals=rows * ff_dim,
                                      bytes_accessed=num_local * 6 * d_model * ff_dim + num_tok * d_model * 6),
        name='expert_block',
    )(meta, gate, pos, digits, tok, w_gate, w_up, w_down)


def pair_kernel(keep, send, out, mine, theirs, send_sem, recv_sem, keep_sem, out_sem):
    me = lax.axis_index('ep')
    other = me + 1 - 2 * lax.rem(me, 2)
    barrier = pltpu.get_barrier_semaphore()
    pl.semaphore_signal(barrier, inc=1, device_id={'ep': other}, device_id_type=pl.DeviceIdType.MESH)
    pl.semaphore_wait(barrier, 1)
    size = keep.shape[0] // PIECES
    remote, local, done = [], [], []
    for p in range(PIECES):
        rows = pl.ds(p * size, size)
        remote.append(pltpu.make_async_remote_copy(
            src_ref=send.at[rows, :], dst_ref=theirs.at[rows, :], send_sem=send_sem.at[p], recv_sem=recv_sem.at[p],
            device_id={'ep': other}, device_id_type=pl.DeviceIdType.MESH))
        local.append(pltpu.make_async_copy(keep.at[rows, :], mine.at[rows, :], keep_sem.at[p]))
        done.append(pltpu.make_async_copy(mine.at[rows, :], out.at[rows, :], out_sem.at[p]))
    for p in range(PIECES):
        remote[p].start()
        local[p].start()
    for p in range(PIECES):
        local[p].wait()
        remote[p].wait_recv()

        def add(i, c, p=p):
            at = pl.ds(pl.multiple_of(p * size + i * 160, 8), 160)
            mine[at, :] = mine[at, :] + theirs[at, :]
            return c

        lax.fori_loop(0, size // 160, add, 0)
        done[p].start()
    for p in range(PIECES):
        remote[p].wait_send()
        done[p].wait()


def pair_sum(keep, send, call_id):
    rows, d_model = keep.shape
    anym = pl.BlockSpec(memory_space=pl.ANY)
    return pl.pallas_call(
        pair_kernel,
        out_shape=jax.ShapeDtypeStruct((rows, d_model), jnp.float32),
        in_specs=[anym, anym],
        out_specs=anym,
        scratch_shapes=[
            pltpu.VMEM((rows, d_model), jnp.float32),
            pltpu.VMEM((rows, d_model), jnp.float32),
            pltpu.SemaphoreType.DMA((PIECES,)),
            pltpu.SemaphoreType.DMA((PIECES,)),
            pltpu.SemaphoreType.DMA((PIECES,)),
            pltpu.SemaphoreType.DMA((PIECES,)),
        ],
        compiler_params=pltpu.CompilerParams(collective_id=call_id, has_side_effects=True, vmem_limit_bytes=67_000_000),
        cost_estimate=pl.CostEstimate(flops=rows * d_model * 4000, transcendentals=0, bytes_accessed=rows * d_model * 16),
        name='pair_sum',
    )(keep, send)


def routing_tables(expert_ids, gate_wts, slot_ids, my_rank, num_local, group_size):
    tok_dev, top_k = expert_ids.shape
    units = tok_dev // UNIT
    key = jnp.where(slot_ids >= 0, expert_ids, -1).astype(jnp.float32).T
    packed = lax.all_gather(jnp.concatenate([key, gate_wts.T], axis=0), 'ep')
    packed = packed.reshape(group_size, 2, top_k, units, UNIT).transpose(1, 2, 0, 3, 4)
    local = (my_rank * num_local + jnp.arange(num_local)).astype(jnp.float32)[:, None, None, None, None]
    hit = packed[0][None] == local
    mask = jnp.any(hit, axis=1)
    gate = jnp.sum(jnp.where(hit, packed[1][None], 0.0), axis=1)

    before = (jnp.arange(UNIT)[:, None] < jnp.arange(UNIT)[None, :]).astype(jnp.bfloat16)
    inner = jnp.einsum('erbk,kl->erbl', mask.astype(jnp.bfloat16), before, preferred_element_type=jnp.float32)
    sums = jnp.sum(mask.astype(jnp.float32), axis=3).reshape(num_local, group_size * units)
    chunk_of_unit = [c for c, n in enumerate(CHUNK_UNITS) for _ in range(n)]
    chunk_of = jnp.tile(jnp.array(chunk_of_unit), group_size)
    block = jnp.arange(group_size * units)
    earlier = (block[:, None] < block[None, :]) & (chunk_of[:, None] == chunk_of[None, :])
    outer = jnp.sum(jnp.where(earlier, sums[:, :, None], 0.0), axis=1).reshape(num_local, group_size, units, 1)
    pos = jnp.where(mask, inner + outer, -1.0).astype(jnp.int32)

    chunks = len(CHUNK_UNITS)
    in_chunk = chunk_of[None, :] == jnp.arange(chunks)[:, None]
    count = jnp.sum(jnp.where(in_chunk[:, None, :], sums[None], 0.0), axis=2).astype(jnp.int32)
    limit = jnp.array([ROW_SIZES[n][-1] for n in CHUNK_UNITS])[:, None]
    passes = (count + limit - 1) // limit
    upto = jnp.arange(num_local)[:, None] <= jnp.arange(num_local)[None, :]
    ends = jnp.sum(jnp.where(upto, passes[:, :, None], 0), axis=1)
    starts = ends - passes
    item = jnp.arange(MAX_ITEMS)
    mine = (starts[:, :, None] <= item) & (item < ends[:, :, None])
    e = jnp.sum(jnp.where(mine, jnp.arange(num_local)[:, None], 0), axis=1)
    p0 = jnp.sum(jnp.where(mine, (item - starts[:, :, None]) * limit[:, :, None], 0), axis=1)
    rows = jnp.minimum(jnp.sum(jnp.where(mine, count[:, :, None], 0), axis=1) - p0, limit)
    extra = jnp.where(item[None, :] == 0, ends[:, -1:], my_rank % 2)
    meta = jnp.concatenate([e, p0, rows, extra], axis=1).astype(jnp.int32)
    tables = []
    unit0 = 0
    for c, n in enumerate(CHUNK_UNITS):
        span = slice(unit0, unit0 + n)
        num_tok = group_size * n * UNIT
        flat_gate = jnp.pad(gate[:, :, span].reshape(num_local * num_tok), (0, 128))
        base = outer[:, :, span, 0].reshape(num_local * group_size * n).astype(jnp.int32)
        tables.append((jnp.concatenate([meta[c], base]), flat_gate, pos[:, :, span].reshape(num_local, 1, num_tok)))
        unit0 += n
    return tables


def solution(mesh):
    group_size = mesh.shape['ep']
    row_spec = P(('dp', 'ep'), None)
    expert_spec = P('ep', None, None)
    same_core = [list(range(core, group_size, 2)) for core in range(2)]

    def layer(tokens, expert_ids, gate_wts, slot_ids, w_gate, w_up, w_down):
        my_rank = lax.axis_index('ep')
        starts = [UNIT * sum(CHUNK_UNITS[:c]) for c in range(len(CHUNK_UNITS) + 1)]
        source = {}
        for members in GATHERS:
            first, last = starts[members[0]], starts[members[-1] + 1]
            whole = lax.all_gather(tokens[first:last], 'ep', axis=0, tiled=False)
            for c in members:
                source[c] = (whole, starts[c] - first)
        tables = routing_tables(expert_ids, gate_wts, slot_ids, my_rank, w_gate.shape[0], group_size)
        outs = []
        last = None

        def reduce(part):
            part = lax.psum_scatter(part, 'ep', scatter_dimension=0, tiled=True, axis_index_groups=same_core)
            return part.reshape(-1, tokens.shape[1]).astype(jnp.bfloat16)

        for c, units in enumerate(CHUNK_UNITS):
            tok, row0 = source[c]
            ids = jnp.arange(group_size * units * UNIT)
            digits = jnp.stack([ids // ID_RADIX, ids % ID_RADIX, jnp.ones_like(ids)] + [jnp.zeros_like(ids)] * 5).astype(jnp.bfloat16)
            meta, gate, pos = tables[c]
            if last is not None:
                meta, last = lax.optimization_barrier((meta, last))
                outs.append(reduce(last))
            last = expert_block(row0, units, meta, gate, pos, digits, tok, w_gate, w_up, w_down)
            last = pair_sum(*last, c)
        outs.append(reduce(last))
        return jnp.concatenate(outs, axis=0)

    return jax.shard_map(layer, mesh=mesh, in_specs=(row_spec, row_spec, row_spec, row_spec, expert_spec, expert_spec, expert_spec), out_specs=row_spec, check_vma=False)
```

```python
import jax
import jax.numpy as jnp
from jax import lax
from jax.experimental import pallas as pl
from jax.experimental.pallas import tpu as pltpu
from jax.sharding import PartitionSpec as P

UNIT = 128
CHUNK_UNITS = (1, 2, 2, 2, 1)
GATHERS = ((0,), (1,), (2, 3, 4))
ROW_SIZES = {1: (160,), 2: (128, 256, 288, 320)}
MAX_ITEMS = 64
FF_BLOCK = 512
FF_PART = 256
OUT_BLOCK = 512
LANES = 128
ID_RADIX = 64
WINDOW = 10
PIECES = 8


def expert_kernel(row0, row_sizes, split, meta, gate, pos, digits, tok_hbm, wg_hbm, wu_hbm, wd_hbm, *refs):
    outs, (tok, acc, wg, wu, wd, onehot, x, h, o, idx_v, idx_s, up_sem, down_sem, tok_sem, idx_sem, out_sem) = refs[:1 + split], refs[1 + split:]
    num_tok, d_model = tok.shape
    shards = tok_hbm.shape[0]
    tc = num_tok // shards
    ff_dim = wg_hbm.shape[2]
    up_steps, down_steps = ff_dim // FF_BLOCK, d_model // OUT_BLOCK
    lines = d_model // LANES
    num_items = meta[3 * MAX_ITEMS]
    parity = meta[3 * MAX_ITEMS + 1]

    def up_copies(item, j):
        cols = pl.ds(pl.multiple_of(j * FF_BLOCK, FF_BLOCK), FF_BLOCK)
        e = meta[item]
        return (pltpu.make_async_copy(wg_hbm.at[e, :, cols], wg.at[j], up_sem.at[j, 0]),
                pltpu.make_async_copy(wu_hbm.at[e, :, cols], wu.at[j], up_sem.at[j, 1]))

    def down_copies(item):
        half = ff_dim // 2
        return [pltpu.make_async_copy(wd_hbm.at[meta[item], pl.ds(k * half, half), :], wd.at[pl.ds(k * half, half), :],
                                      down_sem.at[k]) for k in range(2)]

    def start_all(copies):
        for cp in copies:
            cp.start()

    tok_copies = [pltpu.make_async_copy(tok_hbm.at[s, pl.ds(row0, tc), :], tok.at[pl.ds(s * tc, tc), :], tok_sem.at[s])
                  for s in range(shards)]
    start_all(tok_copies)

    @pl.when(num_items > 0)
    def _():
        for j in range(up_steps):
            start_all(up_copies(0, j))
        start_all(down_copies(0))

    def zero(i, c):
        acc[pl.ds(pl.multiple_of(i * 160, 8), 160), :] = jnp.zeros((160, LANES), jnp.float32)
        return c

    lax.fori_loop(0, acc.shape[0] // 160, zero, 0)
    for cp in tok_copies:
        cp.wait()

    max_rows = row_sizes[-1]
    blocks = num_tok // UNIT

    def block_of(e, p):
        found = -1
        for k in range(blocks):
            found = found + jnp.where(meta[4 * MAX_ITEMS + e * blocks + k] <= p, 1, 0)
        return found

    def dispatch(rows, e, row0, p0, half, first, width):
        start = pl.multiple_of(first * UNIT, UNIT)
        step = 16 if rows % 32 else 32

        def select(i, c):
            row = pl.multiple_of(i * step, step)
            want = lax.broadcasted_iota(jnp.int32, (step, width), 0) + (p0 + row)
            here = pos[e, :, pl.ds(start, width)]
            onehot[pl.ds(row, step), :width] = jnp.where(want == here, 1.0, 0.0).astype(jnp.bfloat16)
            return c

        lax.fori_loop(0, rows // step, select, 0)
        parts = lax.dot_general(digits[:, :width], onehot[:rows, :width], (((1,), (1,)), ((), ())), preferred_element_type=jnp.float32)
        here = parts[0:1] * ID_RADIX + parts[1:2] + (parts[2:3] * start.astype(jnp.float32) + (1.0 - parts[2:3]) * num_tok)
        idx_v[pl.ds(pl.multiple_of(half * 8, 8), 8), :rows] = jnp.broadcast_to(here.astype(jnp.int32), (8, rows))

        def columns(nb, c):
            cols = pl.ds(pl.multiple_of(nb * OUT_BLOCK, OUT_BLOCK), OUT_BLOCK)
            x[pl.ds(pl.multiple_of(row0, 16), rows), cols] = jnp.dot(
                onehot[:rows, :width], tok[pl.ds(start, width), cols], preferred_element_type=jnp.float32).astype(jnp.bfloat16)
            return c

        lax.fori_loop(0, d_model // OUT_BLOCK, columns, 0)

    idx_copy = pltpu.make_async_copy(idx_v, idx_s, idx_sem)
    zero_block = jnp.int32(0)

    def process(m, item):
        def up(j, c):
            for cp in up_copies(item, j):
                cp.wait()

            def part(k, c):
                cols = pl.ds(pl.multiple_of(k * FF_PART, FF_PART), FF_PART)
                a = jnp.dot(x[:m, :], wg[j, :, cols], preferred_element_type=jnp.float32)
                u = jnp.dot(x[:m, :], wu[j, :, cols], preferred_element_type=jnp.float32)
                to = pl.ds(pl.multiple_of(j * FF_BLOCK + k * FF_PART, FF_PART), FF_PART)
                h[:m, to] = (jax.nn.silu(a) * u).astype(jnp.bfloat16)
                return c

            lax.fori_loop(0, FF_BLOCK // FF_PART, part, 0)

            @pl.when(item + 1 < num_items)
            def _():
                start_all(up_copies(item + 1, j))

            return c

        lax.fori_loop(0, up_steps, up, 0)
        for cp in down_copies(item):
            cp.wait()

        def down(j, c):
            cols = pl.ds(pl.multiple_of(j * OUT_BLOCK, OUT_BLOCK), OUT_BLOCK)
            part = jnp.dot(h[:m, :], wd[:, cols], preferred_element_type=jnp.float32)
            for k in range(OUT_BLOCK // LANES):
                o[pl.ds(j * (OUT_BLOCK // LANES) + k, m, stride=lines), :] = part[:, k * LANES:(k + 1) * LANES]
            return c

        lax.fori_loop(0, down_steps, down, 0)

        @pl.when(item + 1 < num_items)
        def _():
            start_all(down_copies(item + 1))

    def scatter(e, rows, half_rows):
        spans = [(at, min(8, lines - at)) for at in range(0, lines, 8)]

        def eight(i, c):
            base = i * 8
            upper = jnp.where(base >= half_rows, 1, 0)
            at0 = base - upper * half_rows
            for half in range(2):
                t = [idx_s[upper * 8, at0 + half * 4 + k] for k in range(4)]
                g = [gate[e * num_tok + t[k]] for k in range(4)]
                new = [[acc[pl.ds(t[k] * lines + at, n), :] + o[pl.ds((base + half * 4 + k) * lines + at, n), :] * g[k]
                        for at, n in spans] for k in range(4)]
                for k in range(4):
                    for (at, n), value in zip(spans, new[k]):
                        acc[pl.ds(t[k] * lines + at, n), :] = value
            return c

        lax.fori_loop(0, (rows + 7) // 8, eight, 0)

    def item_body(item, c):
        e, p0, rows = meta[item], meta[MAX_ITEMS + item], meta[2 * MAX_ITEMS + item]
        half_rows = max_rows
        windowed = False
        starts = (zero_block, zero_block)
        low = 0
        if blocks > WINDOW:
            for m in row_sizes[1:]:
                half_rows = jnp.where(rows <= m, jnp.minimum(half_rows, m // 2), half_rows)
            fits = rows > row_sizes[0]
            starts = []
            for half in range(2):
                begin = p0 + half * half_rows
                end = jnp.minimum(begin + half_rows, p0 + rows) - 1
                first = jnp.minimum(block_of(e, begin), blocks - WINDOW)
                fits = fits & (block_of(e, end) < first + WINDOW)
                starts.append(first)
            windowed = fits
            half_rows = jnp.where(fits, half_rows, max_rows)
            for m in row_sizes[1:]:
                @pl.when(windowed & (half_rows == m // 2))
                def _():
                    def half_step(half, c):
                        first = jnp.where(half == 0, starts[0], starts[1])
                        dispatch(m // 2, e, half * (m // 2), p0 + half * (m // 2), half, first, WINDOW * UNIT)
                        return c

                    lax.fori_loop(0, 2, half_step, 0)

            @pl.when(rows <= row_sizes[0])
            def _():
                dispatch(row_sizes[0], e, 0, p0, 0, zero_block, num_tok)

            @pl.when((rows > row_sizes[0]) & jnp.logical_not(windowed))
            def _():
                dispatch(max_rows, e, 0, p0, 0, zero_block, num_tok)
        else:
            dispatch(max_rows, e, 0, p0, 0, zero_block, num_tok)
        idx_copy.start()
        for m in row_sizes:
            @pl.when((rows > low) & (rows <= m))
            def _():
                process(m, item)

            low = m
        idx_copy.wait()
        scatter(e, rows, half_rows)
        return c

    lax.fori_loop(0, num_items, item_body, 0)
    out_copies = []
    size = tc * lines
    if split:
        for s in range(shards // 2):
            dst = pl.ds(s * size, size)
            mine = pl.ds(pl.multiple_of((2 * s + parity) * size, size), size)
            other = pl.ds(pl.multiple_of((2 * s + 1 - parity) * size, size), size)
            out_copies.append(pltpu.make_async_copy(acc.at[other, :], outs[1].at[dst, :], out_sem.at[s, 0]))
            out_copies.append(pltpu.make_async_copy(acc.at[mine, :], outs[0].at[dst, :], out_sem.at[s, 1]))
    else:
        out_copies.append(pltpu.make_async_copy(acc.at[pl.ds(0, shards * size), :], outs[0], out_sem.at[0, 0]))
    start_all(out_copies)
    for cp in out_copies:
        cp.wait()


def expert_block(row0, units, split, meta, gate, pos, digits, tok, w_gate, w_up, w_down):
    shards, _, d_model = tok.shape
    num_tok = shards * units * UNIT
    num_local, _, ff_dim = w_gate.shape
    smem = pl.BlockSpec(memory_space=pltpu.SMEM)
    vmem = pl.BlockSpec(memory_space=pltpu.VMEM)
    anym = pl.BlockSpec(memory_space=pl.ANY)
    rows = num_tok * 3 // 4
    max_rows = ROW_SIZES[units][-1]
    lines = d_model // LANES
    out = jax.ShapeDtypeStruct((num_tok // (1 + split) * lines, LANES), jnp.float32)
    up_steps = ff_dim // FF_BLOCK

    def body(*refs):
        expert_kernel(row0, ROW_SIZES[units], split, *refs)

    return pl.pallas_call(
        body,
        out_shape=(out,) * (1 + split),
        in_specs=[smem, smem, vmem, vmem, anym, anym, anym, anym],
        out_specs=(anym,) * (1 + split),
        scratch_shapes=[
            pltpu.VMEM((num_tok, d_model), jnp.bfloat16),
            pltpu.VMEM(((num_tok + 8) * lines, LANES), jnp.float32),
            pltpu.VMEM((up_steps, d_model, FF_BLOCK), jnp.bfloat16),
            pltpu.VMEM((up_steps, d_model, FF_BLOCK), jnp.bfloat16),
            pltpu.VMEM((ff_dim, d_model), jnp.bfloat16),
            pltpu.VMEM((max_rows, num_tok), jnp.bfloat16),
            pltpu.VMEM((max_rows, d_model), jnp.bfloat16),
            pltpu.VMEM((max_rows, ff_dim), jnp.bfloat16),
            pltpu.VMEM((max_rows * lines, LANES), jnp.float32),
            pltpu.VMEM((16, max_rows), jnp.int32),
            pltpu.SMEM((16, max_rows), jnp.int32),
            pltpu.SemaphoreType.DMA((up_steps, 2)),
            pltpu.SemaphoreType.DMA((2,)),
            pltpu.SemaphoreType.DMA((shards,)),
            pltpu.SemaphoreType.DMA,
            pltpu.SemaphoreType.DMA((shards // 2, 2)),
        ],
        compiler_params=pltpu.CompilerParams(vmem_limit_bytes=67_000_000),
        cost_estimate=pl.CostEstimate(flops=rows * 6 * d_model * ff_dim * 2, transcendentals=rows * ff_dim,
                                      bytes_accessed=num_local * 6 * d_model * ff_dim + num_tok * d_model * 6),
        name='expert_block',
    )(meta, gate, pos, digits, tok, w_gate, w_up, w_down)


def pair_kernel(keep, send, out, mine, theirs, send_sem, recv_sem, keep_sem, out_sem):
    me = lax.axis_index('ep')
    other = me + 1 - 2 * lax.rem(me, 2)
    barrier = pltpu.get_barrier_semaphore()
    pl.semaphore_signal(barrier, inc=1, device_id={'ep': other}, device_id_type=pl.DeviceIdType.MESH)
    pl.semaphore_wait(barrier, 1)
    size = keep.shape[0] // PIECES
    remote, local, done = [], [], []
    for p in range(PIECES):
        rows = pl.ds(p * size, size)
        remote.append(pltpu.make_async_remote_copy(
            src_ref=send.at[rows, :], dst_ref=theirs.at[rows, :], send_sem=send_sem.at[p], recv_sem=recv_sem.at[p],
            device_id={'ep': other}, device_id_type=pl.DeviceIdType.MESH))
        local.append(pltpu.make_async_copy(keep.at[rows, :], mine.at[rows, :], keep_sem.at[p]))
        done.append(pltpu.make_async_copy(mine.at[rows, :], out.at[rows, :], out_sem.at[p]))
    for p in range(PIECES):
        remote[p].start()
        local[p].start()
    for p in range(PIECES):
        local[p].wait()
        remote[p].wait_recv()

        def add(i, c, p=p):
            at = pl.ds(pl.multiple_of(p * size + i * 160, 8), 160)
            mine[at, :] = mine[at, :] + theirs[at, :]
            return c

        lax.fori_loop(0, size // 160, add, 0)
        done[p].start()
    for p in range(PIECES):
        remote[p].wait_send()
        done[p].wait()


def pair_sum(keep, send, call_id):
    rows, d_model = keep.shape
    anym = pl.BlockSpec(memory_space=pl.ANY)
    return pl.pallas_call(
        pair_kernel,
        out_shape=jax.ShapeDtypeStruct((rows, d_model), jnp.float32),
        in_specs=[anym, anym],
        out_specs=anym,
        scratch_shapes=[
            pltpu.VMEM((rows, d_model), jnp.float32),
            pltpu.VMEM((rows, d_model), jnp.float32),
            pltpu.SemaphoreType.DMA((PIECES,)),
            pltpu.SemaphoreType.DMA((PIECES,)),
            pltpu.SemaphoreType.DMA((PIECES,)),
            pltpu.SemaphoreType.DMA((PIECES,)),
        ],
        compiler_params=pltpu.CompilerParams(collective_id=call_id, has_side_effects=True, vmem_limit_bytes=67_000_000),
        cost_estimate=pl.CostEstimate(flops=rows * d_model * 4000, transcendentals=0, bytes_accessed=rows * d_model * 16),
        name='pair_sum',
    )(keep, send)


def routing_tables(expert_ids, gate_wts, slot_ids, my_rank, num_local, group_size):
    tok_dev, top_k = expert_ids.shape
    units = tok_dev // UNIT
    key = jnp.where(slot_ids >= 0, expert_ids, -1).astype(jnp.float32).T
    packed = lax.all_gather(jnp.concatenate([key, gate_wts.T], axis=0), 'ep')
    packed = packed.reshape(group_size, 2, top_k, units, UNIT).transpose(1, 2, 0, 3, 4)
    local = (my_rank * num_local + jnp.arange(num_local)).astype(jnp.float32)[:, None, None, None, None]
    hit = packed[0][None] == local
    mask = jnp.any(hit, axis=1)
    gate = jnp.sum(jnp.where(hit, packed[1][None], 0.0), axis=1)

    before = (jnp.arange(UNIT)[:, None] < jnp.arange(UNIT)[None, :]).astype(jnp.bfloat16)
    inner = jnp.einsum('erbk,kl->erbl', mask.astype(jnp.bfloat16), before, preferred_element_type=jnp.float32)
    sums = jnp.sum(mask.astype(jnp.float32), axis=3).reshape(num_local, group_size * units)
    chunk_of_unit = [c for c, n in enumerate(CHUNK_UNITS) for _ in range(n)]
    chunk_of = jnp.tile(jnp.array(chunk_of_unit), group_size)
    block = jnp.arange(group_size * units)
    earlier = (block[:, None] < block[None, :]) & (chunk_of[:, None] == chunk_of[None, :])
    outer = jnp.sum(jnp.where(earlier, sums[:, :, None], 0.0), axis=1).reshape(num_local, group_size, units, 1)
    pos = jnp.where(mask, inner + outer, -1.0).astype(jnp.int32)

    chunks = len(CHUNK_UNITS)
    in_chunk = chunk_of[None, :] == jnp.arange(chunks)[:, None]
    count = jnp.sum(jnp.where(in_chunk[:, None, :], sums[None], 0.0), axis=2).astype(jnp.int32)
    limit = jnp.array([ROW_SIZES[n][-1] for n in CHUNK_UNITS])[:, None]
    passes = (count + limit - 1) // limit
    upto = jnp.arange(num_local)[:, None] <= jnp.arange(num_local)[None, :]
    ends = jnp.sum(jnp.where(upto, passes[:, :, None], 0), axis=1)
    starts = ends - passes
    item = jnp.arange(MAX_ITEMS)
    mine = (starts[:, :, None] <= item) & (item < ends[:, :, None])
    e = jnp.sum(jnp.where(mine, jnp.arange(num_local)[:, None], 0), axis=1)
    p0 = jnp.sum(jnp.where(mine, (item - starts[:, :, None]) * limit[:, :, None], 0), axis=1)
    rows = jnp.minimum(jnp.sum(jnp.where(mine, count[:, :, None], 0), axis=1) - p0, limit)
    extra = jnp.where(item[None, :] == 0, ends[:, -1:], my_rank % 2)
    meta = jnp.concatenate([e, p0, rows, extra], axis=1).astype(jnp.int32)
    tables = []
    unit0 = 0
    for c, n in enumerate(CHUNK_UNITS):
        span = slice(unit0, unit0 + n)
        num_tok = group_size * n * UNIT
        flat_gate = jnp.pad(gate[:, :, span].reshape(num_local * num_tok), (0, 128))
        base = outer[:, :, span, 0].reshape(num_local * group_size * n).astype(jnp.int32)
        tables.append((jnp.concatenate([meta[c], base]), flat_gate, pos[:, :, span].reshape(num_local, 1, num_tok)))
        unit0 += n
    return tables


def solution(mesh):
    group_size = mesh.shape['ep']
    row_spec = P(('dp', 'ep'), None)
    expert_spec = P('ep', None, None)
    same_core = [list(range(core, group_size, 2)) for core in range(2)]

    def layer(tokens, expert_ids, gate_wts, slot_ids, w_gate, w_up, w_down):
        my_rank = lax.axis_index('ep')
        starts = [UNIT * sum(CHUNK_UNITS[:c]) for c in range(len(CHUNK_UNITS) + 1)]
        source = {}
        for members in GATHERS:
            first, last = starts[members[0]], starts[members[-1] + 1]
            whole = lax.all_gather(tokens[first:last], 'ep', axis=0, tiled=False)
            for c in members:
                source[c] = (whole, starts[c] - first)
        tables = routing_tables(expert_ids, gate_wts, slot_ids, my_rank, w_gate.shape[0], group_size)
        outs = []
        last = None

        def reduce(part, c):
            part = lax.psum_scatter(part, 'ep', scatter_dimension=0, tiled=True, axis_index_groups=same_core if c > 0 else None)
            return part.reshape(-1, tokens.shape[1]).astype(jnp.bfloat16)

        for c, units in enumerate(CHUNK_UNITS):
            tok, row0 = source[c]
            ids = jnp.arange(group_size * units * UNIT)
            digits = jnp.stack([ids // ID_RADIX, ids % ID_RADIX, jnp.ones_like(ids)] + [jnp.zeros_like(ids)] * 5).astype(jnp.bfloat16)
            meta, gate, pos = tables[c]
            if last is not None:
                meta, last = lax.optimization_barrier((meta, last))
                outs.append(reduce(last, c - 1))
            last = expert_block(row0, units, c > 0, meta, gate, pos, digits, tok, w_gate, w_up, w_down)
            last = pair_sum(*last, c) if c > 0 else last[0]
        outs.append(reduce(last, len(CHUNK_UNITS) - 1))
        return jnp.concatenate(outs, axis=0)

    return jax.shard_map(layer, mesh=mesh, in_specs=(row_spec, row_spec, row_spec, row_spec, expert_spec, expert_spec, expert_spec), out_specs=row_spec, check_vma=False)
```
